256 devices in a mesh: dp: 8 (over z), expert: 32 (over x, y, core).
Axes of the slice: x: 4, y: 4, z: 8, core: 2. Of those that a mesh axis runs over, the one named last changes fastest.
Arguments:
- tokens: bfloat16 [65536, 2048], P(('dp', 'expert')), may hold values from -6 to 6
- expert_ranks: int32 [32, 65536], P(None, ('dp', 'expert')), may hold values from 0 to 65535, as said below
- capacity: int32 [32], replicated, may hold values from 512 to 1024, as said below
- weight_in: bfloat16 [32, 2048, 8192], P('expert', None, 'dp'), may hold values from -0.125 to 0.125
- weight_out: bfloat16 [32, 8192, 2048], P('expert', 'dp'), may hold values from -0.0625 to 0.0625
- gate_weights: float32 [32, 1024], P('expert', 'dp'), may hold values from 0.05 to 1
Outputs:
- combined: bfloat16 [65536, 2048], P(('dp', 'expert'))
The draws below stay inside these ranges and needn't reach their ends.
Inputs may be any that keep to these rules, and one draw needn't show every extreme that they name: `expert_ranks`: for each expert the ranks are a permutation of 0 to 65535. Of the 256 tokens of one device, at most 8 have rank under 1024 for one expert; for an expert of capacity 1024, some devices have exactly 8. At least one expert has capacity 1024.
All inputs are finite; a program needn't handle non-finite values.
Results may differ from the reference program's by a relative error of at most 0.0053.
Values may be sent and summed in bfloat16 or wider, within the bound.
No kernel may reach another device: no remote copies, remote signals or barrier semaphores. Data moves between devices by JAX's collectives and lax.ppermute only.
A program may use at most 64 MiB of HBM per device.

```python
import math
import jax
import jax.numpy as jnp
from jax import lax

D = 2048
FF = 8192
TOK_DEV = 256
EXPERTS = 32
TOKENS = 65536
CAP = 1024


def local_permutation(subkey):
    return jax.random.permutation(subkey, TOK_DEV)


def device_permutation(subkey):
    return jax.random.permutation(subkey, TOKENS // TOK_DEV)


def token_permutation(subkey):
    return jax.random.permutation(subkey, TOKENS)


def draw_expert_ranks(key, part):
    devices_all = TOKENS // TOK_DEV
    average = TOK_DEV // 64
    low_total = 3 * average // 2
    key_mid = jax.random.fold_in(key, 11)
    key_low = jax.random.fold_in(key, 12)
    key_order = jax.random.fold_in(key, 13)
    key_local = jax.random.fold_in(key, 14)
    key_ties = jax.random.fold_in(key, 15)
    position = lax.broadcasted_iota(jnp.int32, (EXPERTS, devices_all), 1)
    paired = position // 2
    leading = position % 2 == 0
    middle_draw = jax.random.randint(key_mid, (EXPERTS, devices_all // 2), average // 2, average + average // 2 + 1)
    low_draw = jax.random.randint(key_low, (EXPERTS, devices_all // 2), average // 4, low_total - average // 4 + 1)
    middle_pick = jnp.take_along_axis(middle_draw, paired, axis=1)
    low_pick = jnp.take_along_axis(low_draw, paired, axis=1)
    middle_value = jnp.where(leading, middle_pick, 2 * average - middle_pick)
    low_value = jnp.where(leading, low_pick, low_total - low_pick)
    pattern = jnp.where(position < devices_all // 8, 2 * average, jnp.where(position < devices_all // 2, middle_value, low_value))
    orders = jax.vmap(device_permutation)(jax.random.split(key_order, EXPERTS))
    quota = jnp.take_along_axis(pattern, orders, axis=1).astype(jnp.int32)
    locals_all = jax.vmap(local_permutation)(jax.random.split(key_local, EXPERTS * devices_all))
    locals_all = locals_all.reshape(EXPERTS, devices_all, TOK_DEV)
    selected = (locals_all < quota[:, :, None]).reshape(EXPERTS, TOKENS)
    ties = jax.vmap(token_permutation)(jax.random.split(key_ties, EXPERTS)).astype(jnp.int32)
    score = jnp.where(selected, ties, TOKENS + ties).astype(jnp.int32)
    order = jnp.argsort(score, axis=1, stable=True)
    ranks = jnp.argsort(order, axis=1, stable=True)
    return ranks.astype(jnp.int32)


def draw_capacity(key, part):
    key_values = jax.random.fold_in(key, 21)
    key_full = jax.random.fold_in(key, 22)
    values = jax.random.randint(key_values, (EXPERTS,), CAP // 2, CAP + 1)
    full_index = jax.random.randint(key_full, (), 0, EXPERTS)
    position = lax.broadcasted_iota(jnp.int32, (EXPERTS,), 0)
    return jnp.where(position == full_index, CAP, values).astype(jnp.int32)


def shard_levels(key, shape, cuts, smallest, top_value):
    loudness = 1.0
    for axis_at, parts in cuts:
        steps = jax.random.uniform(jax.random.fold_in(jax.random.fold_in(key, 6), axis_at), (parts,), jnp.float32, smallest / len(cuts), top_value / len(cuts))
        loudness = loudness * jnp.repeat(jnp.exp(steps), shape[axis_at] // parts).reshape((-1,) + (1,) * (len(shape) - 1 - axis_at))
    return loudness


def gaussian(stream_key, shape, width, most, cuts=(), kind=jnp.bfloat16):
    result = jax.random.normal(stream_key, shape, jnp.float32) * width
    if len(cuts) > 0:
        result = shard_levels(stream_key, shape, cuts, -0.22, 0.18) * result
    return jnp.clip(result, min=-most, max=most).astype(kind)


def setup_inputs(seed: int = 0) -> dict:
    key_list = jax.random.split(jax.random.key(seed), 7)
    tokens = gaussian(key_list[0], (TOKENS, D), 1.0, 6.0, ((0, 256),))
    expert_ranks = draw_expert_ranks(jax.random.fold_in(key_list[6], 71), 0)
    capacity = draw_capacity(jax.random.fold_in(key_list[6], 71), 0)
    weight_in = gaussian(key_list[3], (EXPERTS, D, FF), D ** -0.5, 0.125, ((0, 32), (2, 8)))
    weight_out = gaussian(key_list[4], (EXPERTS, FF, D), FF ** -0.5, 0.0625, ((0, 32), (1, 8)))
    gate_weights = jnp.clip(jnp.exp(math.log(1.0) - 2.9957323 * jax.random.uniform(key_list[5], (EXPERTS, CAP), jnp.float32) ** shard_levels(key_list[5], (EXPERTS, CAP), ((0, 32), (1, 8)), -0.2, 0.2)), 0.05, 1.0)
    return {"tokens": tokens, "expert_ranks": expert_ranks, "capacity": capacity, "weight_in": weight_in, "weight_out": weight_out, "gate_weights": gate_weights}


def reference(tokens, expert_ranks, capacity, weight_in, weight_out, gate_weights):
    total = tokens.shape[0]
    tokens_wide = tokens.astype(jnp.float32)

    def one_expert(accum, index):
        rank_row = lax.dynamic_index_in_dim(expert_ranks, index, 0, keepdims=False)
        limit = lax.dynamic_index_in_dim(capacity, index, 0, keepdims=False)
        chosen = rank_row < limit
        chosen_int = chosen.astype(jnp.int32)
        slots = (jnp.cumsum(chosen_int).astype(jnp.int32) - chosen_int).astype(jnp.int32)
        target = jnp.where(chosen, slots, CAP).astype(jnp.int32)
        slot_rows = jnp.zeros((CAP + 1, D), jnp.float32).at[target].add(tokens_wide)[:CAP].astype(jnp.bfloat16)
        first_weight = lax.dynamic_index_in_dim(weight_in, index, 0, keepdims=False)
        second_weight = lax.dynamic_index_in_dim(weight_out, index, 0, keepdims=False)
        hidden = jnp.maximum(jnp.dot(slot_rows, first_weight, preferred_element_type=jnp.float32), 0.0).astype(jnp.bfloat16)
        expert_out = jnp.dot(hidden, second_weight, preferred_element_type=jnp.float32)
        gates = lax.dynamic_index_in_dim(gate_weights, index, 0, keepdims=False)
        scaled = (gates[:, None] * expert_out).astype(jnp.bfloat16)
        picked = jnp.take(scaled, jnp.minimum(slots, CAP - 1).astype(jnp.int32), axis=0)
        accum = accum + jnp.where(chosen[:, None], picked.astype(jnp.float32), 0.0)
        return accum, None

    accum, unused = lax.scan(one_expert, jnp.zeros((total, D), jnp.float32), jnp.arange(EXPERTS, dtype=jnp.int32))
    return accum.astype(jnp.bfloat16)
```

```python
import jax
import jax.numpy as jnp
from jax import lax
from jax.sharding import Mesh
from jax.sharding import PartitionSpec as P

MOST = 8
EXPERT = ("expert_0", "expert_1", "expert_2")
DP_EXPERT = ("dp", "expert_0", "expert_1", "expert_2")


def exclusive(values):
    return jnp.cumsum(values) - values


def on_device(tokens, expert_ranks, capacity, weight_in, weight_out, gate_weights):
    dp_count = lax.axis_size("dp")
    expert_count = lax.axis_size(EXPERT)
    token_count, width = tokens.shape
    slots_dp = gate_weights.shape[1]
    rows_all = expert_count * MOST
    own_dp = lax.axis_index("dp")
    own_expert = lax.axis_index(EXPERT)

    chosen = expert_ranks < capacity[:, None]
    chosen_int = chosen.astype(jnp.int32)
    counts = jnp.sum(chosen_int, axis=1)
    before = jnp.cumsum(chosen_int, axis=1) - chosen_int
    places = lax.broadcasted_iota(jnp.int32, (expert_count, MOST, token_count), 1)
    pack_table = jnp.logical_and(chosen[:, None, :], before[:, None, :] == places)
    pack_table = pack_table.astype(jnp.bfloat16).reshape(rows_all, token_count)
    packed = jnp.dot(pack_table, tokens, preferred_element_type=jnp.float32).astype(jnp.bfloat16)
    arrived_rows = lax.all_to_all(
        packed.reshape(expert_count, MOST, width), EXPERT, split_axis=0, concat_axis=0, tiled=True
    ).reshape(rows_all, width)

    device_ids = lax.broadcasted_iota(jnp.int32, (expert_count, expert_count), 0)
    expert_ids = lax.broadcasted_iota(jnp.int32, (expert_count, expert_count), 1)
    table = lax.psum(jnp.where(device_ids == own_expert, counts[None, :], 0), EXPERT)
    plane_ids = lax.broadcasted_iota(jnp.int32, (dp_count, expert_count), 0)
    plane_counts = lax.psum(
        jnp.where(plane_ids == own_dp, jnp.sum(table, axis=0)[None, :], 0), "dp"
    )
    most_rows = jnp.max(plane_counts)
    arrived = jnp.sum(jnp.where(expert_ids == own_expert, table, 0), axis=1)
    earlier = jnp.logical_and(plane_ids < own_dp, expert_ids[:dp_count] == own_expert)
    first_slot = jnp.sum(jnp.where(earlier, plane_counts, 0))
    within = lax.broadcasted_iota(jnp.int32, (expert_count, MOST), 1)
    target = jnp.where(
        within < arrived[:, None], exclusive(arrived)[:, None] + within, -1
    ).reshape(rows_all)
    gates_all = lax.all_gather(gate_weights[0], "dp", axis=0, tiled=True)
    gates_all = jnp.concatenate([gates_all, jnp.zeros((rows_all,), gates_all.dtype)])

    def experts(rows, plane_rows):
        slot_ids = lax.broadcasted_iota(jnp.int32, (rows_all, plane_rows), 1)
        place_table = (target[:, None] == slot_ids).astype(jnp.bfloat16)
        plane = lax.dot_general(
            place_table, rows, (((0,), (0,)), ((), ())), preferred_element_type=jnp.float32
        ).astype(jnp.bfloat16)
        slot_rows = lax.all_gather(plane, "dp", axis=0, tiled=True)
        hidden = jnp.maximum(
            jnp.dot(slot_rows, weight_in[0], preferred_element_type=jnp.float32), 0.0
        ).astype(jnp.bfloat16)
        share = jnp.dot(hidden, weight_out[0], preferred_element_type=jnp.float32)
        out = lax.psum_scatter(
            share.astype(jnp.bfloat16), "dp", scatter_dimension=0, tiled=True
        ).astype(jnp.float32)
        gates = lax.dynamic_slice_in_dim(gates_all, first_slot, plane_rows, 0)
        scaled = (gates[:, None] * out).astype(jnp.bfloat16)
        returned = jnp.dot(place_table, scaled, preferred_element_type=jnp.float32)
        return returned.astype(jnp.bfloat16)

    fair = slots_dp + slots_dp // 4
    sent_back = lax.cond(
        most_rows <= fair,
        lambda rows: experts(rows, fair),
        lambda rows: experts(rows, rows_all),
        arrived_rows,
    )
    results = lax.all_to_all(
        sent_back.reshape(expert_count, MOST, width), EXPERT, split_axis=0, concat_axis=0, tiled=True
    ).reshape(rows_all, width)
    combined = lax.dot_general(
        pack_table, results, (((0,), (0,)), ((), ())), preferred_element_type=jnp.float32
    )
    return combined.astype(jnp.bfloat16)


def solution(mesh):
    split = Mesh(
        mesh.devices.reshape(mesh.shape["dp"], 4, 4, 2), ("dp", "expert_0", "expert_1", "expert_2")
    )
    placed = (
        P(DP_EXPERT, None),
        P(None, DP_EXPERT),
        P(),
        P(EXPERT, None, "dp"),
        P(EXPERT, "dp", None),
        P(EXPERT, "dp"),
    )
    return jax.shard_map(
        on_device, mesh=split, in_specs=placed, out_specs=P(DP_EXPERT, None), check_vma=False
    )
```

```python
import jax
import jax.numpy as jnp
from jax import lax
from jax.sharding import Mesh
from jax.sharding import PartitionSpec as P

MOST = 8
LANES = 128
EXPERT = ("expert_0", "expert_1", "expert_2")
DP_EXPERT = ("dp", "expert_0", "expert_1", "expert_2")


def exclusive(values):
    return jnp.cumsum(values) - values


def on_device(tokens, expert_ranks, capacity, weight_in, weight_out, gate_weights):
    dp_count = lax.axis_size("dp")
    expert_count = lax.axis_size(EXPERT)
    token_count, width = tokens.shape
    slots_dp = gate_weights.shape[1]
    rows_all = expert_count * MOST
    own_dp = lax.axis_index("dp")
    own_expert = lax.axis_index(EXPERT)

    chosen = expert_ranks < capacity[:, None]
    chosen_int = chosen.astype(jnp.int32)
    counts = jnp.sum(chosen_int, axis=1)
    before = jnp.cumsum(chosen_int, axis=1) - chosen_int
    places = lax.broadcasted_iota(jnp.int32, (expert_count, MOST, token_count), 1)
    pack_table = jnp.logical_and(chosen[:, None, :], before[:, None, :] == places)
    pack_table = pack_table.astype(jnp.bfloat16).reshape(rows_all, token_count)
    packed = jnp.dot(pack_table, tokens, preferred_element_type=jnp.float32).astype(jnp.bfloat16)
    arrived_rows = lax.all_to_all(
        packed.reshape(expert_count, MOST, width), EXPERT, split_axis=0, concat_axis=0, tiled=True
    ).reshape(rows_all, width)

    device_ids = lax.broadcasted_iota(jnp.int32, (expert_count, expert_count), 0)
    expert_ids = lax.broadcasted_iota(jnp.int32, (expert_count, expert_count), 1)
    table = jnp.where(device_ids == own_expert, counts[None, :], 0)
    table = lax.psum(table.reshape(-1, LANES), EXPERT).reshape(expert_count, expert_count)
    arrived = jnp.sum(jnp.where(expert_ids == own_expert, table, 0), axis=1)
    plane_ids = lax.broadcasted_iota(jnp.int32, (dp_count, LANES), 0)
    lane_ids = lax.broadcasted_iota(jnp.int32, (dp_count, LANES), 1)
    plane_row = jnp.pad(jnp.sum(table, axis=0).astype(jnp.float32), (0, LANES - expert_count))
    both = jnp.concatenate(
        [
            jnp.where(plane_ids == own_dp, plane_row[None, :], 0.0),
            jnp.where(plane_ids == own_dp, gate_weights.reshape(-1, LANES), 0.0),
        ]
    )
    both = lax.psum(both, "dp")
    plane_counts = both[:dp_count].astype(jnp.int32)
    most_rows = jnp.max(plane_counts)
    earlier = jnp.logical_and(plane_ids < own_dp, lane_ids == own_expert)
    first_slot = jnp.sum(jnp.where(earlier, plane_counts, 0))
    gates_all = jnp.concatenate(
        [both[dp_count:].reshape(-1), jnp.zeros((rows_all,), jnp.float32)]
    )
    within = lax.broadcasted_iota(jnp.int32, (expert_count, MOST), 1)
    target = jnp.where(
        within < arrived[:, None], exclusive(arrived)[:, None] + within, -1
    ).reshape(rows_all)

    def experts(rows, plane_rows):
        slot_ids = lax.broadcasted_iota(jnp.int32, (rows_all, plane_rows), 1)
        place_table = (target[:, None] == slot_ids).astype(jnp.bfloat16)
        plane = lax.dot_general(
            place_table, rows, (((0,), (0,)), ((), ())), preferred_element_type=jnp.float32
        ).astype(jnp.bfloat16)
        slot_rows = lax.all_gather(plane, "dp", axis=0, tiled=True)
        hidden = jnp.maximum(
            jnp.dot(slot_rows, weight_in[0], preferred_element_type=jnp.float32), 0.0
        ).astype(jnp.bfloat16)
        share = jnp.dot(hidden, weight_out[0], preferred_element_type=jnp.float32)
        out = lax.psum_scatter(
            share.astype(jnp.bfloat16), "dp", scatter_dimension=0, tiled=True
        ).astype(jnp.float32)
        gates = lax.dynamic_slice_in_dim(gates_all, first_slot, plane_rows, 0)
        scaled = (gates[:, None] * out).astype(jnp.bfloat16)
        returned = jnp.dot(place_table, scaled, preferred_element_type=jnp.float32)
        return returned.astype(jnp.bfloat16)

    fair = slots_dp + slots_dp // 4
    sent_back = lax.cond(
        most_rows <= fair,
        lambda rows: experts(rows, fair),
        lambda rows: experts(rows, rows_all),
        arrived_rows,
    )
    results = lax.all_to_all(
        sent_back.reshape(expert_count, MOST, width), EXPERT, split_axis=0, concat_axis=0, tiled=True
    ).reshape(rows_all, width)
    combined = lax.dot_general(
        pack_table, results, (((0,), (0,)), ((), ())), preferred_element_type=jnp.float32
    )
    return combined.astype(jnp.bfloat16)


def solution(mesh):
    split = Mesh(
        mesh.devices.reshape(mesh.shape["dp"], 4, 4, 2), ("dp", "expert_0", "expert_1", "expert_2")
    )
    placed = (
        P(DP_EXPERT, None),
        P(None, DP_EXPERT),
        P(),
        P(EXPERT, None, "dp"),
        P(EXPERT, "dp", None),
        P(EXPERT, "dp"),
    )
    return jax.shard_map(
        on_device, mesh=split, in_specs=placed, out_specs=P(DP_EXPERT, None), check_vma=False
    )
```

```python
import jax
import jax.numpy as jnp
from jax import lax
from jax.sharding import Mesh
from jax.sharding import PartitionSpec as P

MOST = 8
LANES = 128
EXPERT = ("expert_0", "expert_1", "expert_2")
DP_EXPERT = ("dp", "expert_0", "expert_1", "expert_2")


def exclusive(values):
    return jnp.cumsum(values) - values


def ring_experts(plane, first_weight, second_weight, dp_count):
    far = dp_count // 2
    half = plane.shape[0] // 2
    upward = [(i, (i + 1) % dp_count) for i in range(dp_count)]
    downward = [(i, (i - 1) % dp_count) for i in range(dp_count)]

    def up(rows):
        return lax.ppermute(rows, "dp", upward)

    def down(rows):
        return lax.ppermute(rows, "dp", downward)

    def mlp(*pieces):
        rows = jnp.concatenate(pieces)
        hidden = jnp.maximum(jnp.dot(rows, first_weight, preferred_element_type=jnp.float32), 0.0)
        out = jnp.dot(hidden.astype(jnp.bfloat16), second_weight, preferred_element_type=jnp.float32)
        return out

    def parts(out):
        return [out[i * half : (i + 1) * half] for i in range(4)]

    top, bottom = plane[:half], plane[half:]
    up_top, down_bottom = up(top), down(bottom)
    up_bottom, down_top = up(bottom), down(top)
    outs = {}
    for k in range(1, far):
        if k > 1:
            up_top, down_bottom, outs[k - 1] = lax.optimization_barrier((up_top, down_bottom, outs[k - 1]))
        next_up_top, next_down_bottom = up(up_top), down(down_bottom)
        if k < far - 1:
            next_up_bottom, next_down_top = up(up_bottom), down(down_top)
        outs[k] = mlp(up_top, up_bottom, down_top, down_bottom)
        up_top, down_bottom, up_bottom, down_top = next_up_top, next_down_bottom, next_up_bottom, next_down_top

    def narrow(rows):
        return rows.astype(jnp.bfloat16)

    def wide(rows):
        return rows.astype(jnp.float32)

    below_top, _, _, above_bottom = parts(outs[far - 1])
    send_up, send_down = narrow(above_bottom), narrow(below_top)
    up_top, down_bottom, send_up, send_down = lax.optimization_barrier(
        (up_top, down_bottom, send_up, send_down)
    )
    up_bottom, down_top = up(send_up), down(send_down)
    last = parts(mlp(up_top, top, bottom, down_bottom))
    send_up, send_down = narrow(last[0]), narrow(last[3])
    up_top, down_bottom = up(send_up), down(send_down)
    for k in range(far - 1, 0, -1):
        below_top, below_bottom, above_top, above_bottom = parts(outs[k])
        if k < far - 1:
            up_bottom, down_top, send_up, send_down = lax.optimization_barrier(
                (up_bottom, down_top, send_up, send_down)
            )
            send_up, send_down = narrow(wide(up_bottom) + above_bottom), narrow(wide(down_top) + below_top)
            next_up_bottom, next_down_top = up(send_up), down(send_down)
        else:
            next_up_bottom, next_down_top = up_bottom, down_top
        up_top, down_bottom, send_up, send_down = lax.optimization_barrier(
            (up_top, down_bottom, send_up, send_down)
        )
        send_up, send_down = narrow(wide(up_top) + above_top), narrow(wide(down_bottom) + below_bottom)
        up_top, down_bottom = up(send_up), down(send_down)
        up_bottom, down_top = next_up_bottom, next_down_top
    return jnp.concatenate(
        [last[1] + wide(up_top) + wide(down_top), last[2] + wide(up_bottom) + wide(down_bottom)]
    )


def on_device(tokens, expert_ranks, capacity, weight_in, weight_out, gate_weights):
    dp_count = lax.axis_size("dp")
    expert_count = lax.axis_size(EXPERT)
    token_count, width = tokens.shape
    slots_dp = gate_weights.shape[1]
    rows_all = expert_count * MOST
    own_dp = lax.axis_index("dp")
    own_expert = lax.axis_index(EXPERT)

    chosen = expert_ranks < capacity[:, None]
    chosen_int = chosen.astype(jnp.int32)
    counts = jnp.sum(chosen_int, axis=1)
    before = jnp.cumsum(chosen_int, axis=1) - chosen_int
    places = lax.broadcasted_iota(jnp.int32, (expert_count, MOST, token_count), 1)
    pack_table = jnp.logical_and(chosen[:, None, :], before[:, None, :] == places)
    pack_table = pack_table.astype(jnp.bfloat16).reshape(rows_all, token_count)
    packed = jnp.dot(pack_table, tokens, preferred_element_type=jnp.float32).astype(jnp.bfloat16)
    arrived_rows = lax.all_to_all(
        packed.reshape(expert_count, MOST, width), EXPERT, split_axis=0, concat_axis=0, tiled=True
    ).reshape(rows_all, width)

    device_ids = lax.broadcasted_iota(jnp.int32, (expert_count, expert_count), 0)
    expert_ids = lax.broadcasted_iota(jnp.int32, (expert_count, expert_count), 1)
    table = jnp.where(device_ids == own_expert, counts[None, :], 0)
    table = lax.optimization_barrier(table.reshape(-1, LANES))
    table = lax.optimization_barrier(lax.psum(table, EXPERT)).reshape(expert_count, expert_count)
    arrived = jnp.sum(jnp.where(expert_ids == own_expert, table, 0), axis=1)
    plane_ids = lax.broadcasted_iota(jnp.int32, (dp_count, LANES), 0)
    lane_ids = lax.broadcasted_iota(jnp.int32, (dp_count, LANES), 1)
    plane_row = jnp.pad(jnp.sum(table, axis=0).astype(jnp.float32), (0, LANES - expert_count))
    both = jnp.concatenate(
        [
            jnp.where(plane_ids == own_dp, plane_row[None, :], 0.0),
            jnp.where(plane_ids == own_dp, gate_weights.reshape(-1, LANES), 0.0),
        ]
    )
    both = lax.psum(both, "dp")
    plane_counts = both[:dp_count].astype(jnp.int32)
    most_rows = jnp.max(plane_counts)
    earlier = jnp.logical_and(plane_ids < own_dp, lane_ids == own_expert)
    first_slot = jnp.sum(jnp.where(earlier, plane_counts, 0))
    gates_all = jnp.concatenate(
        [both[dp_count:].reshape(-1), jnp.zeros((2 * rows_all,), jnp.float32)]
    )
    within = lax.broadcasted_iota(jnp.int32, (expert_count, MOST), 1)
    target = jnp.where(
        within < arrived[:, None], exclusive(arrived)[:, None] + within, -1
    ).reshape(rows_all)

    round_rows = slots_dp + slots_dp // 4

    def experts(state):
        step, sent_back = state
        first = step * round_rows
        slot_ids = first + lax.broadcasted_iota(jnp.int32, (rows_all, round_rows), 1)
        place_table = (target[:, None] == slot_ids).astype(jnp.bfloat16)
        plane = lax.dot_general(
            place_table, arrived_rows, (((0,), (0,)), ((), ())), preferred_element_type=jnp.float32
        ).astype(jnp.bfloat16)
        out = ring_experts(plane, weight_in[0], weight_out[0], dp_count)
        gates = lax.dynamic_slice_in_dim(gates_all, first_slot + first, round_rows, 0)
        scaled = (gates[:, None] * out).astype(jnp.bfloat16)
        returned = jnp.dot(place_table, scaled, preferred_element_type=jnp.float32)
        return step + 1, sent_back + returned.astype(jnp.bfloat16)

    rounds, sent_back = lax.while_loop(
        lambda state: state[0] * round_rows < most_rows,
        experts,
        (jnp.int32(0), jnp.zeros((rows_all, width), jnp.bfloat16)),
    )
    results = lax.all_to_all(
        sent_back.reshape(expert_count, MOST, width), EXPERT, split_axis=0, concat_axis=0, tiled=True
    ).reshape(rows_all, width)
    combined = lax.dot_general(
        pack_table, results, (((0,), (0,)), ((), ())), preferred_element_type=jnp.float32
    )
    return combined.astype(jnp.bfloat16)


def solution(mesh):
    split = Mesh(
        mesh.devices.reshape(mesh.shape["dp"], 4, 4, 2), ("dp", "expert_0", "expert_1", "expert_2")
    )
    placed = (
        P(DP_EXPERT, None),
        P(None, DP_EXPERT),
        P(),
        P(EXPERT, None, "dp"),
        P(EXPERT, "dp", None),
        P(EXPERT, "dp"),
    )
    return jax.shard_map(
        on_device, mesh=split, in_specs=placed, out_specs=P(DP_EXPERT, None), check_vma=False
    )
```

```python
import jax
import jax.numpy as jnp
from jax import lax
from jax.experimental import pallas as pl
from jax.experimental.pallas import tpu as pltpu
from jax.sharding import Mesh
from jax.sharding import PartitionSpec as P


MOST = 8
LANES = 128
NOTE = 8
HIDDEN_BLOCK = 256
VMEM_LIMIT = 20 * 1024 * 1024
EXPERT = ("expert_0", "expert_1", "expert_2")
DP_EXPERT = ("dp", "expert_0", "expert_1", "expert_2")


def narrow(rows):
    return rows.astype(jnp.bfloat16)


def wide(rows):
    return rows.astype(jnp.float32)


def expert_kernel(*refs):
    *refs, rows_ref, sums_ref = refs
    count = (len(refs) - 2) // 2
    pieces, (first_ref, second_ref), outs = refs[:count], refs[count : count + 2], refs[count + 2 :]
    half = outs[0].shape[0]
    step = pl.program_id(0)

    @pl.when(step == 0)
    def _():
        for i, piece in enumerate(pieces):
            rows_ref[i * half : (i + 1) * half] = piece[piece.shape[0] - half :]

    hidden = jnp.dot(rows_ref[...], first_ref[...], preferred_element_type=jnp.float32)
    hidden = jnp.maximum(hidden, 0.0).astype(jnp.bfloat16)
    sums = jnp.dot(hidden, second_ref[...], preferred_element_type=jnp.float32)

    @pl.when(step == 0)
    def _():
        sums_ref[...] = sums

    @pl.when(jnp.logical_and(step > 0, step < pl.num_programs(0) - 1))
    def _():
        sums_ref[...] += sums

    @pl.when(step == pl.num_programs(0) - 1)
    def _():
        for i, out in enumerate(outs):
            part = slice(i * half, (i + 1) * half)
            out[...] = (sums_ref[part] + sums[part]).astype(out.dtype)


def expert_rows(pieces, first_weight, second_weight, half, kinds):
    width, hidden = first_weight.shape
    count = len(pieces) * half
    return pl.pallas_call(
        expert_kernel,
        grid=(hidden // HIDDEN_BLOCK,),
        in_specs=[
            *[pl.BlockSpec(piece.shape, lambda i: (0, 0)) for piece in pieces],
            pl.BlockSpec((width, HIDDEN_BLOCK), lambda i: (0, i)),
            pl.BlockSpec((HIDDEN_BLOCK, width), lambda i: (i, 0)),
        ],
        out_specs=[pl.BlockSpec((half, width), lambda i: (0, 0)) for _ in pieces],
        out_shape=[pltpu.HBM((half, width), kind) for kind in kinds],
        scratch_shapes=[pltpu.VMEM((count, width), jnp.bfloat16), pltpu.VMEM((count, width), jnp.float32)],
        compiler_params=pltpu.CompilerParams(
            dimension_semantics=("arbitrary",), vmem_limit_bytes=VMEM_LIMIT
        ),
        cost_estimate=pl.CostEstimate(
            flops=4 * count * width * hidden,
            transcendentals=0,
            bytes_accessed=4 * width * hidden + 6 * count * width,
        ),
        name="expert_rows",
    )(*pieces, first_weight, second_weight)


def ring_experts(note, plane, first_weight, second_weight, dp_count):
    far = dp_count // 2
    half = plane.shape[0] // 2
    upward = [(i, (i + 1) % dp_count) for i in range(dp_count)]
    downward = [(i, (i - 1) % dp_count) for i in range(dp_count)]

    def hop(up_rows, down_rows):
        up_rows = lax.ppermute(up_rows, "dp", upward)
        down_rows = lax.ppermute(down_rows, "dp", downward)
        return up_rows, down_rows

    def mlp(*pieces, sent=()):
        kinds = [jnp.bfloat16 if i in sent else jnp.float32 for i in range(len(pieces))]
        return expert_rows(pieces, first_weight, second_weight, half, kinds)

    def after(rows, *others):
        return lax.optimization_barrier((rows, others))[0]

    top, bottom = jnp.concatenate([note, plane[:half]]), plane[half:]
    kept = 4 * LANES
    notes = {0: note[:1, :kept]}
    firsts = hop(top, bottom)
    seconds = hop(bottom, top)
    outs, done = {}, ()
    for k in range(1, far):
        firsts = after(firsts, *done)
        seconds = after(seconds, *firsts)
        notes[-k % dp_count], notes[k] = firsts[0][:1, :kept], seconds[1][:1, :kept]
        next_firsts = hop(*firsts)
        if k < far - 1:
            next_seconds = hop(*seconds)
        outs[k] = mlp(firsts[0], seconds[0], seconds[1], firsts[1], sent=(0, 3) if k == far - 1 else ())
        done = *outs[k], notes[-k % dp_count], notes[k]
        firsts, seconds = next_firsts, next_seconds

    below_top, below_bottom, above_top, above_bottom = outs[far - 1]
    seconds = hop(above_bottom, below_top)
    firsts = after(firsts, above_bottom, below_top, *done)
    notes[far] = firsts[0][:1, :kept]
    last = mlp(firsts[0], top, bottom, firsts[1], sent=(0, 3))
    sends = last[0], last[3]
    firsts = hop(*sends)
    for k in range(far - 1, 0, -1):
        if k > 1:
            below_top, _, _, above_bottom = outs[k - 1]
            seconds = after(seconds, *sends)
            sends = narrow(wide(seconds[0]) + above_bottom), narrow(wide(seconds[1]) + below_top)
            seconds = hop(*sends)
        _, below_bottom, above_top, _ = outs[k]
        firsts = after(firsts, *sends)
        sends = narrow(wide(firsts[0]) + above_top), narrow(wide(firsts[1]) + below_bottom)
        firsts = hop(*sends)
    sums = jnp.concatenate(
        [last[1] + wide(firsts[0]) + wide(seconds[1]), last[2] + wide(seconds[0]) + wide(firsts[1])]
    )
    return sums, after([notes[j] for j in range(dp_count)], *sends)


def on_device(tokens, expert_ranks, capacity, weight_in, weight_out, gate_weights):
    dp_count = lax.axis_size("dp")
    expert_count = lax.axis_size(EXPERT)
    token_count, width = tokens.shape
    slots_dp = gate_weights.shape[1]
    rows_all = expert_count * MOST
    round_rows = slots_dp + slots_dp // 4
    own_dp = lax.axis_index("dp")

    chosen = expert_ranks < capacity[:, None]
    chosen_int = chosen.astype(jnp.int32)
    before = jnp.cumsum(chosen_int, axis=1) - chosen_int
    places = lax.broadcasted_iota(jnp.int32, (expert_count, MOST, token_count), 1)
    pack_table = jnp.logical_and(chosen[:, None, :], before[:, None, :] == places)
    pack_table = pack_table.astype(jnp.bfloat16).reshape(rows_all, token_count)
    marked = jnp.concatenate([tokens, jnp.ones((token_count, LANES), jnp.bfloat16)], axis=1)
    packed = jnp.dot(pack_table, marked, preferred_element_type=jnp.float32).astype(jnp.bfloat16)
    arrived = lax.all_to_all(
        packed.reshape(expert_count, MOST, width + LANES), EXPERT, split_axis=0, concat_axis=0, tiled=True
    ).reshape(rows_all, width + LANES)
    arrived_rows, taken = arrived[:, :width], arrived[:, width:]

    earlier = lax.broadcasted_iota(jnp.int32, (rows_all, rows_all), 1) < lax.broadcasted_iota(
        jnp.int32, (rows_all, rows_all), 0
    )
    place = jnp.dot(earlier.astype(jnp.bfloat16), taken, preferred_element_type=jnp.float32)
    target = jnp.where(taken > 0, place, -1.0)
    plane_count = (place + wide(taken))[rows_all - 1 :]

    gate_high = lax.reduce_precision(gate_weights, 8, 7)
    gate_left = gate_weights - gate_high
    gate_middle = lax.reduce_precision(gate_left, 8, 7)
    gate_low = gate_left - gate_middle
    note = jnp.concatenate([gate_high, gate_middle, gate_low, plane_count], axis=1).astype(jnp.bfloat16)
    note = jnp.pad(note, ((0, NOTE - 1), (0, width - note.shape[1])))

    def experts(state):
        step, _, sent_back = state
        first = step * round_rows
        slot_ids = first + lax.broadcasted_iota(jnp.int32, (rows_all, round_rows), 1)
        place_table = (target[:, :1] == slot_ids.astype(jnp.float32)).astype(jnp.bfloat16)
        plane = lax.dot_general(
            place_table, arrived_rows, (((0,), (0,)), ((), ())), preferred_element_type=jnp.float32
        ).astype(jnp.bfloat16)
        sums, notes = ring_experts(note, plane, weight_in[0], weight_out[0], dp_count)
        table = jnp.concatenate(notes).astype(jnp.float32)
        table = lax.dynamic_slice_in_dim(
            jnp.concatenate([table, table]), (dp_count - own_dp) % dp_count, dp_count, 0
        )
        gates = table[:, :slots_dp] + table[:, slots_dp : 2 * slots_dp] + table[:, 2 * slots_dp : 3 * slots_dp]
        plane_counts = table[:, 3 * slots_dp].astype(jnp.int32)
        first_slot = jnp.sum(
            jnp.where(lax.broadcasted_iota(jnp.int32, (dp_count,), 0) < own_dp, plane_counts, 0)
        )
        gates = jnp.pad(gates.reshape(-1), (0, 2 * rows_all))
        gates = lax.dynamic_slice_in_dim(gates, first_slot + first, round_rows, 0)
        scaled = (gates[:, None] * sums).astype(jnp.bfloat16)
        returned = jnp.dot(place_table, scaled, preferred_element_type=jnp.float32)
        return step + 1, jnp.max(plane_counts), sent_back + returned.astype(jnp.bfloat16)

    _, _, sent_back = lax.while_loop(
        lambda state: state[0] * round_rows < state[1],
        experts,
        (jnp.int32(0), jnp.int32(1), jnp.zeros((rows_all, width), jnp.bfloat16)),
    )
    results = lax.all_to_all(
        sent_back.reshape(expert_count, MOST, width), EXPERT, split_axis=0, concat_axis=0, tiled=True
    ).reshape(rows_all, width)
    combined = lax.dot_general(
        pack_table, results, (((0,), (0,)), ((), ())), preferred_element_type=jnp.float32
    )
    return combined.astype(jnp.bfloat16)


def solution(mesh):
    split = Mesh(
        mesh.devices.reshape(mesh.shape["dp"], 4, 4, 2), ("dp", "expert_0", "expert_1", "expert_2")
    )
    placed = (
        P(DP_EXPERT, None),
        P(None, DP_EXPERT),
        P(),
        P(EXPERT, None, "dp"),
        P(EXPERT, "dp", None),
        P(EXPERT, "dp"),
    )
    return jax.shard_map(
        on_device, mesh=split, in_specs=placed, out_specs=P(DP_EXPERT, None), check_vma=False
    )
```

```python
import jax
import jax.numpy as jnp
from jax import lax
from jax.experimental import pallas as pl
from jax.experimental.pallas import tpu as pltpu
from jax.sharding import Mesh
from jax.sharding import PartitionSpec as P


MOST = 8
LANES = 128
NOTE = 8
HIDDEN_BLOCK = 512
OUT_BLOCK = 512
VMEM_LIMIT = 20 * 1024 * 1024
EXPERT = ("expert_0", "expert_1", "expert_2")
DP_EXPERT = ("dp", "expert_0", "expert_1", "expert_2")


def narrow(rows):
    return rows.astype(jnp.bfloat16)


def wide(rows):
    return rows.astype(jnp.float32)


def expert_kernel(*refs):
    *refs, rows_ref, hidden_ref = refs
    count = (len(refs) - 2) // 2
    pieces, (first_ref, second_ref), outs = refs[:count], refs[count : count + 2], refs[count + 2 :]
    half, width = outs[0].shape
    for i, piece in enumerate(pieces):
        rows_ref[i * half : (i + 1) * half] = piece[piece.shape[0] - half :]

    def hidden_block(i, _):
        block = pl.ds(pl.multiple_of(i * HIDDEN_BLOCK, HIDDEN_BLOCK), HIDDEN_BLOCK)
        hidden = jnp.dot(rows_ref[...], first_ref[:, block], preferred_element_type=jnp.float32)
        hidden_ref[:, block] = jnp.maximum(hidden, 0.0).astype(jnp.bfloat16)
        return 0

    def out_block(i, _):
        block = pl.ds(pl.multiple_of(i * OUT_BLOCK, OUT_BLOCK), OUT_BLOCK)
        sums = jnp.dot(hidden_ref[...], second_ref[:, block], preferred_element_type=jnp.float32)
        for j, out in enumerate(outs):
            out[:, block] = sums[j * half : (j + 1) * half].astype(out.dtype)
        return 0

    lax.fori_loop(0, hidden_ref.shape[1] // HIDDEN_BLOCK, hidden_block, 0)
    lax.fori_loop(0, width // OUT_BLOCK, out_block, 0)


def expert_rows(pieces, first_weight, second_weight, half, kinds):
    width, hidden = first_weight.shape
    count = len(pieces) * half
    return pl.pallas_call(
        expert_kernel,
        out_shape=[jax.ShapeDtypeStruct((half, width), kind) for kind in kinds],
        scratch_shapes=[pltpu.VMEM((count, width), jnp.bfloat16), pltpu.VMEM((count, hidden), jnp.bfloat16)],
        compiler_params=pltpu.CompilerParams(vmem_limit_bytes=VMEM_LIMIT),
        cost_estimate=pl.CostEstimate(
            flops=4 * count * width * hidden,
            transcendentals=0,
            bytes_accessed=4 * width * hidden + 6 * count * width,
        ),
        name="expert_rows",
    )(*pieces, first_weight, second_weight)


def ring_experts(note, plane, first_weight, second_weight, dp_count):
    far = dp_count // 2
    half = plane.shape[0] // 2
    upward = [(i, (i + 1) % dp_count) for i in range(dp_count)]
    downward = [(i, (i - 1) % dp_count) for i in range(dp_count)]

    def hop(up_rows, down_rows):
        up_rows = lax.ppermute(up_rows, "dp", upward)
        down_rows = lax.ppermute(down_rows, "dp", downward)
        return up_rows, down_rows

    def mlp(*pieces, sent=()):
        kinds = [jnp.bfloat16 if i in sent else jnp.float32 for i in range(len(pieces))]
        return expert_rows(pieces, first_weight, second_weight, half, kinds)

    def after(rows, *others):
        return lax.optimization_barrier((rows, others))[0]

    top, bottom = jnp.concatenate([note, plane[:half]]), plane[half:]
    kept = 4 * LANES
    notes = {0: note[:1, :kept]}
    firsts = hop(top, bottom)
    seconds = hop(bottom, top)
    outs, done = {}, ()
    for k in range(1, far):
        firsts = after(firsts, *done)
        seconds = after(seconds, *firsts)
        notes[-k % dp_count], notes[k] = firsts[0][:1, :kept], seconds[1][:1, :kept]
        next_firsts = hop(*firsts)
        if k < far - 1:
            next_seconds = hop(*seconds)
        outs[k] = mlp(firsts[0], seconds[0], seconds[1], firsts[1], sent=(0, 3) if k == far - 1 else ())
        done = *outs[k], notes[-k % dp_count], notes[k]
        firsts, seconds = next_firsts, next_seconds

    below_top, below_bottom, above_top, above_bottom = outs[far - 1]
    seconds = hop(above_bottom, below_top)
    firsts = after(firsts, above_bottom, below_top, *done)
    notes[far] = firsts[0][:1, :kept]
    last = mlp(firsts[0], top, bottom, firsts[1], sent=(0, 3))
    sends = last[0], last[3]
    firsts = hop(*sends)
    for k in range(far - 1, 0, -1):
        if k > 1:
            below_top, _, _, above_bottom = outs[k - 1]
            seconds = after(seconds, *sends)
            sends = narrow(wide(seconds[0]) + above_bottom), narrow(wide(seconds[1]) + below_top)
            seconds = hop(*sends)
        _, below_bottom, above_top, _ = outs[k]
        firsts = after(firsts, *sends)
        sends = narrow(wide(firsts[0]) + above_top), narrow(wide(firsts[1]) + below_bottom)
        firsts = hop(*sends)
    sums = jnp.concatenate(
        [last[1] + wide(firsts[0]) + wide(seconds[1]), last[2] + wide(seconds[0]) + wide(firsts[1])]
    )
    return sums, after([notes[j] for j in range(dp_count)], *sends)


def on_device(tokens, expert_ranks, capacity, weight_in, weight_out, gate_weights):
    dp_count = lax.axis_size("dp")
    expert_count = lax.axis_size(EXPERT)
    token_count, width = tokens.shape
    slots_dp = gate_weights.shape[1]
    rows_all = expert_count * MOST
    round_rows = slots_dp + slots_dp // 4
    own_dp = lax.axis_index("dp")

    chosen = expert_ranks < capacity[:, None]
    chosen_int = chosen.astype(jnp.int32)
    before = jnp.cumsum(chosen_int, axis=1) - chosen_int
    places = lax.broadcasted_iota(jnp.int32, (expert_count, MOST, token_count), 1)
    pack_table = jnp.logical_and(chosen[:, None, :], before[:, None, :] == places)
    pack_table = pack_table.astype(jnp.bfloat16).reshape(rows_all, token_count)
    marked = jnp.concatenate([tokens, jnp.ones((token_count, LANES), jnp.bfloat16)], axis=1)
    packed = jnp.dot(pack_table, marked, preferred_element_type=jnp.float32).astype(jnp.bfloat16)
    arrived = lax.all_to_all(
        packed.reshape(expert_count, MOST, width + LANES), EXPERT, split_axis=0, concat_axis=0, tiled=True
    ).reshape(rows_all, width + LANES)
    arrived_rows, taken = arrived[:, :width], arrived[:, width:]

    earlier = lax.broadcasted_iota(jnp.int32, (rows_all, rows_all), 1) < lax.broadcasted_iota(
        jnp.int32, (rows_all, rows_all), 0
    )
    place = jnp.dot(earlier.astype(jnp.bfloat16), taken, preferred_element_type=jnp.float32)
    target = jnp.where(taken > 0, place, -1.0)
    plane_count = (place + wide(taken))[rows_all - 1 :]

    gate_high = lax.reduce_precision(gate_weights, 8, 7)
    gate_left = gate_weights - gate_high
    gate_middle = lax.reduce_precision(gate_left, 8, 7)
    gate_low = gate_left - gate_middle
    note = jnp.concatenate([gate_high, gate_middle, gate_low, plane_count], axis=1).astype(jnp.bfloat16)
    note = jnp.pad(note, ((0, NOTE - 1), (0, width - note.shape[1])))

    def experts(state):
        step, _, sent_back = state
        first = step * round_rows
        slot_ids = first + lax.broadcasted_iota(jnp.int32, (rows_all, round_rows), 1)
        place_table = (target[:, :1] == slot_ids.astype(jnp.float32)).astype(jnp.bfloat16)
        plane = lax.dot_general(
            place_table, arrived_rows, (((0,), (0,)), ((), ())), preferred_element_type=jnp.float32
        ).astype(jnp.bfloat16)
        sums, notes = ring_experts(note, plane, weight_in[0], weight_out[0], dp_count)
        table = jnp.concatenate(notes).astype(jnp.float32)
        table = lax.dynamic_slice_in_dim(
            jnp.concatenate([table, table]), (dp_count - own_dp) % dp_count, dp_count, 0
        )
        gates = table[:, :slots_dp] + table[:, slots_dp : 2 * slots_dp] + table[:, 2 * slots_dp : 3 * slots_dp]
        plane_counts = table[:, 3 * slots_dp].astype(jnp.int32)
        first_slot = jnp.sum(
            jnp.where(lax.broadcasted_iota(jnp.int32, (dp_count,), 0) < own_dp, plane_counts, 0)
        )
        gates = jnp.pad(gates.reshape(-1), (0, 2 * rows_all))
        gates = lax.dynamic_slice_in_dim(gates, first_slot + first, round_rows, 0)
        scaled = (gates[:, None] * sums).astype(jnp.bfloat16)
        returned = jnp.dot(place_table, scaled, preferred_element_type=jnp.float32)
        return step + 1, jnp.max(plane_counts), sent_back + returned.astype(jnp.bfloat16)

    _, _, sent_back = lax.while_loop(
        lambda state: state[0] * round_rows < state[1],
        experts,
        (jnp.int32(0), jnp.int32(1), jnp.zeros((rows_all, width), jnp.bfloat16)),
    )
    results = lax.all_to_all(
        sent_back.reshape(expert_count, MOST, width), EXPERT, split_axis=0, concat_axis=0, tiled=True
    ).reshape(rows_all, width)
    combined = lax.dot_general(
        pack_table, results, (((0,), (0,)), ((), ())), preferred_element_type=jnp.float32
    )
    return combined.astype(jnp.bfloat16)


def solution(mesh):
    split = Mesh(
        mesh.devices.reshape(mesh.shape["dp"], 4, 4, 2), ("dp", "expert_0", "expert_1", "expert_2")
    )
    placed = (
        P(DP_EXPERT, None),
        P(None, DP_EXPERT),
        P(),
        P(EXPERT, None, "dp"),
        P(EXPERT, "dp", None),
        P(EXPERT, "dp"),
    )
    return jax.shard_map(
        on_device, mesh=split, in_specs=placed, out_specs=P(DP_EXPERT, None), check_vma=False
    )
```

```python
import jax
import jax.numpy as jnp
from jax import lax
from jax.experimental import pallas as pl
from jax.experimental.pallas import tpu as pltpu
from jax.sharding import Mesh
from jax.sharding import PartitionSpec as P


MOST = 8
LANES = 128
NOTE = 8
BLOCK = 512
VMEM_LIMIT = 20 * 1024 * 1024
EXPERT = ("expert_0", "expert_1", "expert_2")
DP_EXPERT = ("dp", "expert_0", "expert_1", "expert_2")


def narrow(rows):
    return rows.astype(jnp.bfloat16)


def wide(rows):
    return rows.astype(jnp.float32)


def gather_rows(pieces, rows_ref, half):
    for i, piece in enumerate(pieces):
        rows_ref[i * half : (i + 1) * half] = piece[piece.shape[0] - half :]


def expert_sums(first_ref, second_ref, outs, rows_ref, hidden_ref, first_block, second_block):
    half, width = outs[0].shape

    def hidden_block(i, _):
        block = first_block(i)
        hidden = jnp.dot(rows_ref[...], first_ref[:, block], preferred_element_type=jnp.float32)
        hidden_ref[:, block] = jnp.maximum(hidden, 0.0).astype(jnp.bfloat16)
        return 0

    def out_block(i, _):
        block = second_block(i)
        sums = jnp.dot(hidden_ref[...], second_ref[:, block], preferred_element_type=jnp.float32)
        for j, out in enumerate(outs):
            out[:, block] = sums[j * half : (j + 1) * half].astype(out.dtype)
        return 0

    lax.fori_loop(0, hidden_ref.shape[1] // BLOCK, hidden_block, 0)
    lax.fori_loop(0, width // BLOCK, out_block, 0)


def columns(i):
    return pl.ds(pl.multiple_of(i * BLOCK, BLOCK), BLOCK)


def split_refs(refs):
    count = (len(refs) - 2) // 2
    return refs[:count], refs[count], refs[count + 1], refs[count + 2 :]


def expert_kernel(*refs):
    *refs, rows_ref, hidden_ref = refs
    pieces, first_ref, second_ref, outs = split_refs(refs)
    gather_rows(pieces, rows_ref, outs[0].shape[0])
    expert_sums(first_ref, second_ref, outs, rows_ref, hidden_ref, columns, columns)


def staged_expert_kernel(*refs):
    *refs, rows_ref, hidden_ref, first_ref, second_ref, first_sems, second_sems = refs
    pieces, first_far, second_far, outs = split_refs(refs)

    def first_copy(i):
        return pltpu.make_async_copy(first_far.at[:, columns(i)], first_ref.at[:, columns(i)], first_sems.at[i])

    def second_copy(i):
        return pltpu.make_async_copy(second_far.at[:, columns(i)], second_ref.at[:, columns(i)], second_sems.at[i])

    def first_block(i):
        first_copy(i).wait()
        return columns(i)

    def second_block(i):
        second_copy(i).wait()
        return columns(i)

    for i in range(first_ref.shape[1] // BLOCK):
        first_copy(i).start()
    for i in range(second_ref.shape[1] // BLOCK):
        second_copy(i).start()
    gather_rows(pieces, rows_ref, outs[0].shape[0])
    expert_sums(first_ref, second_ref, outs, rows_ref, hidden_ref, first_block, second_block)


def expert_rows(pieces, first_weight, second_weight, half, kinds, staged):
    width, hidden = first_weight.shape
    count = len(pieces) * half
    scratch = [pltpu.VMEM((count, width), jnp.bfloat16), pltpu.VMEM((count, hidden), jnp.bfloat16)]
    specs = {}
    if staged:
        scratch += [
            pltpu.VMEM(first_weight.shape, jnp.bfloat16),
            pltpu.VMEM(second_weight.shape, jnp.bfloat16),
            pltpu.SemaphoreType.DMA((hidden // BLOCK,)),
            pltpu.SemaphoreType.DMA((width // BLOCK,)),
        ]
        near, far = pl.BlockSpec(memory_space=pltpu.VMEM), pl.BlockSpec(memory_space=pl.ANY)
        specs = {"in_specs": [near] * len(pieces) + [far] * 2}
    return pl.pallas_call(
        staged_expert_kernel if staged else expert_kernel,
        out_shape=[jax.ShapeDtypeStruct((half, width), kind) for kind in kinds],
        scratch_shapes=scratch,
        compiler_params=pltpu.CompilerParams(vmem_limit_bytes=VMEM_LIMIT),
        cost_estimate=pl.CostEstimate(
            flops=4 * count * width * hidden,
            transcendentals=0,
            bytes_accessed=4 * width * hidden + 6 * count * width,
        ),
        name="expert_rows",
        **specs,
    )(*pieces, first_weight, second_weight)


def pack_kernel(tokens_ref, ranks_ref, capacity_ref, packed_ref, table_ref, blank_ref):
    experts, count = ranks_ref.shape
    width = tokens_ref.shape[1]
    chosen = ranks_ref[...] < capacity_ref[...]
    earlier = lax.broadcasted_iota(jnp.int32, (count, count), 0) < lax.broadcasted_iota(
        jnp.int32, (count, count), 1
    )
    before = jnp.dot(
        jnp.where(chosen, 1.0, 0.0).astype(jnp.bfloat16),
        jnp.where(earlier, 1.0, 0.0).astype(jnp.bfloat16),
        preferred_element_type=jnp.float32,
    )
    place = jnp.where(chosen, before, -1.0)
    row = lax.broadcasted_iota(jnp.int32, (MOST, count), 0).astype(jnp.float32)
    for e in range(experts):
        table_ref[e * MOST : (e + 1) * MOST] = jnp.where(place[e : e + 1] == row, 1.0, 0.0).astype(jnp.bfloat16)
    table = table_ref[...]
    packed = jnp.dot(table, tokens_ref[...], preferred_element_type=jnp.float32)
    packed_ref[:, :width] = packed.astype(jnp.bfloat16)
    blank_ref[...] = jnp.zeros(blank_ref.shape, blank_ref.dtype)
    ones = jnp.ones((count, LANES), jnp.bfloat16)
    packed_ref[:, width:] = jnp.dot(table, ones, preferred_element_type=jnp.float32).astype(jnp.bfloat16)


def pack(tokens, expert_ranks, capacity):
    count, width = tokens.shape
    rows_all = expert_ranks.shape[0] * MOST
    return pl.pallas_call(
        pack_kernel,
        out_shape=[
            jax.ShapeDtypeStruct((rows_all, width + LANES), jnp.bfloat16),
            pltpu.HBM((rows_all, count), jnp.bfloat16),
            pltpu.HBM((rows_all, width), jnp.bfloat16),
        ],
        compiler_params=pltpu.CompilerParams(vmem_limit_bytes=VMEM_LIMIT),
        name="pack",
    )(tokens, expert_ranks, capacity[:, None])


def finish_kernel(*refs):
    *parts, gates_ref, target_ref, kept_ref, out_ref, scaled_ref = refs
    half = parts[0].shape[0]
    for i, (own, one, other) in enumerate((parts[:3], parts[3:])):
        rows = slice(i * half, (i + 1) * half)
        sums = own[...] + wide(one[...]) + wide(other[...])
        scaled_ref[rows] = narrow(gates_ref[rows] * sums)
    target = target_ref[:, :1]
    count = 2 * half
    slots = lax.broadcasted_iota(jnp.int32, (target.shape[0], count), 1).astype(jnp.float32)
    table = jnp.where(target == slots, 1.0, 0.0).astype(jnp.bfloat16)
    returned = jnp.dot(table, scaled_ref[...], preferred_element_type=jnp.float32)
    here = jnp.logical_and(target >= 0.0, target < count)
    out_ref[...] = narrow(jnp.where(here, returned, wide(kept_ref[...])))


def finish(parts, gates, target, kept):
    half, width = parts[0].shape
    return pl.pallas_call(
        finish_kernel,
        out_shape=jax.ShapeDtypeStruct(kept.shape, kept.dtype),
        scratch_shapes=[pltpu.VMEM((2 * half, width), jnp.bfloat16)],
        compiler_params=pltpu.CompilerParams(vmem_limit_bytes=VMEM_LIMIT),
        name="finish",
    )(*parts, gates, target, kept)


def ring_experts(note, plane, first_weight, second_weight, dp_count):
    far = dp_count // 2
    half = plane.shape[0] // 2
    upward = [(i, (i + 1) % dp_count) for i in range(dp_count)]
    downward = [(i, (i - 1) % dp_count) for i in range(dp_count)]

    def hop(up_rows, down_rows):
        up_rows = lax.ppermute(up_rows, "dp", upward)
        down_rows = lax.ppermute(down_rows, "dp", downward)
        return up_rows, down_rows

    def mlp(*pieces, sent=(), staged=False):
        kinds = [jnp.bfloat16 if i in sent else jnp.float32 for i in range(len(pieces))]
        return expert_rows(pieces, first_weight, second_weight, half, kinds, staged)

    def after(rows, *others):
        return lax.optimization_barrier((rows, others))[0]

    top, bottom = jnp.concatenate([note, plane[:half]]), plane[half:]
    kept = 4 * LANES
    notes = {0: note[:1, :kept]}
    firsts = hop(top, bottom)
    seconds = hop(bottom, top)
    outs, done = {}, ()
    for k in range(1, far):
        firsts = after(firsts, *done)
        seconds = after(seconds, *firsts)
        notes[-k % dp_count], notes[k] = firsts[0][:1, :kept], seconds[1][:1, :kept]
        next_firsts = hop(*firsts)
        if k < far - 1:
            next_seconds = hop(*seconds)
        outs[k] = mlp(firsts[0], seconds[0], seconds[1], firsts[1], sent=(0, 3) if k == far - 1 else (), staged=k == 1)
        done = *outs[k], notes[-k % dp_count], notes[k]
        firsts, seconds = next_firsts, next_seconds

    below_top, below_bottom, above_top, above_bottom = outs[far - 1]
    seconds = hop(above_bottom, below_top)
    firsts = after(firsts, above_bottom, below_top, *done)
    notes[far] = firsts[0][:1, :kept]
    last = mlp(firsts[0], top, bottom, firsts[1], sent=(0, 3))
    sends = last[0], last[3]
    firsts = hop(*sends)
    for k in range(far - 1, 0, -1):
        if k > 1:
            below_top, _, _, above_bottom = outs[k - 1]
            seconds = after(seconds, *sends)
            sends = narrow(wide(seconds[0]) + above_bottom), narrow(wide(seconds[1]) + below_top)
            seconds = hop(*sends)
        _, below_bottom, above_top, _ = outs[k]
        firsts = after(firsts, *sends)
        sends = narrow(wide(firsts[0]) + above_top), narrow(wide(firsts[1]) + below_bottom)
        firsts = hop(*sends)
    parts = last[1], firsts[0], seconds[1], last[2], seconds[0], firsts[1]
    return parts, after([notes[j] for j in range(dp_count)], *sends)


def on_device(tokens, expert_ranks, capacity, weight_in, weight_out, gate_weights):
    dp_count = lax.axis_size("dp")
    expert_count = lax.axis_size(EXPERT)
    width = tokens.shape[1]
    slots_dp = gate_weights.shape[1]
    rows_all = expert_count * MOST
    round_rows = slots_dp + slots_dp // 4
    own_dp = lax.axis_index("dp")

    packed, pack_table, blank = pack(tokens, expert_ranks, capacity)
    arrived = lax.all_to_all(
        packed.reshape(expert_count, MOST, width + LANES), EXPERT, split_axis=0, concat_axis=0, tiled=True
    ).reshape(rows_all, width + LANES)
    taken = arrived[:, width:]

    earlier = lax.broadcasted_iota(jnp.int32, (rows_all, rows_all), 1) < lax.broadcasted_iota(
        jnp.int32, (rows_all, rows_all), 0
    )
    place = jnp.dot(earlier.astype(jnp.bfloat16), taken, preferred_element_type=jnp.float32)
    target = jnp.where(taken > 0, place, -1.0)
    plane_count = (place + wide(taken))[rows_all - 1 :]

    gate_high = lax.reduce_precision(gate_weights, 8, 7)
    gate_left = gate_weights - gate_high
    gate_middle = lax.reduce_precision(gate_left, 8, 7)
    gate_low = gate_left - gate_middle
    note = jnp.concatenate([gate_high, gate_middle, gate_low, plane_count], axis=1).astype(jnp.bfloat16)
    note = jnp.pad(note, ((0, NOTE - 1), (0, width - note.shape[1])))

    def experts(state):
        step, _, sent_back = state
        first = step * round_rows
        here = target - first.astype(jnp.float32)
        slot_ids = lax.broadcasted_iota(jnp.int32, (rows_all, round_rows), 1)
        place_table = (here[:, :1] == slot_ids.astype(jnp.float32)).astype(jnp.bfloat16)
        plane = lax.dot_general(
            place_table, arrived[:, :width], (((0,), (0,)), ((), ())), preferred_element_type=jnp.float32
        ).astype(jnp.bfloat16)
        parts, notes = ring_experts(note, plane, weight_in[0], weight_out[0], dp_count)
        table = jnp.concatenate(notes).astype(jnp.float32)
        table = lax.dynamic_slice_in_dim(
            jnp.concatenate([table, table]), (dp_count - own_dp) % dp_count, dp_count, 0
        )
        gates = table[:, :slots_dp] + table[:, slots_dp : 2 * slots_dp] + table[:, 2 * slots_dp : 3 * slots_dp]
        plane_counts = table[:, 3 * slots_dp].astype(jnp.int32)
        first_slot = jnp.sum(
            jnp.where(lax.broadcasted_iota(jnp.int32, (dp_count,), 0) < own_dp, plane_counts, 0)
        )
        gates = jnp.pad(gates.reshape(-1), (0, 2 * rows_all))
        gates = lax.dynamic_slice_in_dim(gates, first_slot + first, round_rows, 0)
        sent_back = finish(parts, gates[:, None], here, sent_back)
        return step + 1, jnp.max(plane_counts), sent_back

    _, _, sent_back = lax.while_loop(
        lambda state: state[0] * round_rows < state[1],
        experts,
        (jnp.int32(0), jnp.int32(1), blank),
    )
    results = lax.all_to_all(
        sent_back.reshape(expert_count, MOST, width), EXPERT, split_axis=0, concat_axis=0, tiled=True
    ).reshape(rows_all, width)
    combined = lax.dot_general(
        pack_table, results, (((0,), (0,)), ((), ())), preferred_element_type=jnp.float32
    )
    return combined.astype(jnp.bfloat16)


def solution(mesh):
    split = Mesh(
        mesh.devices.reshape(mesh.shape["dp"], 4, 4, 2), ("dp", "expert_0", "expert_1", "expert_2")
    )
    placed = (
        P(DP_EXPERT, None),
        P(None, DP_EXPERT),
        P(),
        P(EXPERT, None, "dp"),
        P(EXPERT, "dp", None),
        P(EXPERT, "dp"),
    )
    return jax.shard_map(
        on_device, mesh=split, in_specs=placed, out_specs=P(DP_EXPERT, None), check_vma=False
    )
```

```python
import jax
import jax.numpy as jnp
from jax import lax
from jax.experimental import pallas as pl
from jax.experimental.pallas import tpu as pltpu
from jax.sharding import Mesh
from jax.sharding import PartitionSpec as P


MOST = 8
LANES = 128
NOTE = 8
BLOCK = 512
VMEM_LIMIT = 20 * 1024 * 1024
EXPERT = ("expert_0", "expert_1", "expert_2")
DP_EXPERT = ("dp", "expert_0", "expert_1", "expert_2")


def narrow(rows):
    return rows.astype(jnp.bfloat16)


def wide(rows):
    return rows.astype(jnp.float32)


def gather_rows(pieces, rows_ref, half):
    for i, piece in enumerate(pieces):
        rows_ref[i * half : (i + 1) * half] = piece[piece.shape[0] - half :]


def expert_sums(first_ref, second_ref, outs, rows_ref, hidden_ref, first_block, second_block):
    half, width = outs[0].shape

    def hidden_block(i, _):
        block = first_block(i)
        hidden = jnp.dot(rows_ref[...], first_ref[:, block], preferred_element_type=jnp.float32)
        hidden_ref[:, block] = jnp.maximum(hidden, 0.0).astype(jnp.bfloat16)
        return 0

    def out_block(i, _):
        block = second_block(i)
        sums = jnp.dot(hidden_ref[...], second_ref[:, block], preferred_element_type=jnp.float32)
        for j, out in enumerate(outs):
            out[:, block] = sums[j * half : (j + 1) * half].astype(out.dtype)
        return 0

    lax.fori_loop(0, hidden_ref.shape[1] // BLOCK, hidden_block, 0)
    lax.fori_loop(0, width // BLOCK, out_block, 0)


def columns(i):
    return pl.ds(pl.multiple_of(i * BLOCK, BLOCK), BLOCK)


def split_refs(refs):
    count = (len(refs) - 2) // 2
    return refs[:count], refs[count], refs[count + 1], refs[count + 2 :]


def expert_kernel(*refs):
    *refs, rows_ref, hidden_ref = refs
    pieces, first_ref, second_ref, outs = split_refs(refs)
    gather_rows(pieces, rows_ref, outs[0].shape[0])
    expert_sums(first_ref, second_ref, outs, rows_ref, hidden_ref, columns, columns)


def staged_expert_kernel(*refs):
    *refs, first_ref, second_ref, rows_ref, hidden_ref, first_sems, second_sems = refs
    pieces, first_far, second_far, outs = split_refs(refs)

    def first_copy(i):
        return pltpu.make_async_copy(first_far.at[:, columns(i)], first_ref.at[:, columns(i)], first_sems.at[i])

    def second_copy(i):
        return pltpu.make_async_copy(second_far.at[:, columns(i)], second_ref.at[:, columns(i)], second_sems.at[i])

    def first_block(i):
        first_copy(i).wait()
        return columns(i)

    def second_block(i):
        second_copy(i).wait()
        return columns(i)

    for i in range(first_ref.shape[1] // BLOCK):
        first_copy(i).start()
    for i in range(second_ref.shape[1] // BLOCK):
        second_copy(i).start()
    gather_rows(pieces, rows_ref, outs[0].shape[0])
    expert_sums(first_ref, second_ref, outs, rows_ref, hidden_ref, first_block, second_block)


def expert_rows(pieces, first_weight, second_weight, half, kinds, staged):
    width, hidden = first_weight.shape
    count = len(pieces) * half
    scratch = [pltpu.VMEM((count, width), jnp.bfloat16), pltpu.VMEM((count, hidden), jnp.bfloat16)]
    out_shape = [jax.ShapeDtypeStruct((half, width), kind) for kind in kinds]
    specs = {}
    if staged:
        scratch += [
            pltpu.SemaphoreType.DMA((hidden // BLOCK,)),
            pltpu.SemaphoreType.DMA((width // BLOCK,)),
        ]
        out_shape += [pltpu.VMEM(w.shape, w.dtype) for w in (first_weight, second_weight)]
        near, far = pl.BlockSpec(memory_space=pltpu.VMEM), pl.BlockSpec(memory_space=pl.ANY)
        specs = {"in_specs": [near] * len(pieces) + [far] * 2, "out_specs": [near] * len(out_shape)}
    return pl.pallas_call(
        staged_expert_kernel if staged else expert_kernel,
        out_shape=out_shape,
        scratch_shapes=scratch,
        compiler_params=pltpu.CompilerParams(vmem_limit_bytes=VMEM_LIMIT),
        cost_estimate=pl.CostEstimate(
            flops=4 * count * width * hidden,
            transcendentals=0,
            bytes_accessed=4 * width * hidden + 6 * count * width,
        ),
        name="expert_rows",
        **specs,
    )(*pieces, first_weight, second_weight)


def pack_kernel(tokens_ref, ranks_ref, capacity_ref, packed_ref, table_ref, blank_ref):
    experts, count = ranks_ref.shape
    width = tokens_ref.shape[1]
    chosen = ranks_ref[...] < capacity_ref[...]
    earlier = lax.broadcasted_iota(jnp.int32, (count, count), 0) < lax.broadcasted_iota(
        jnp.int32, (count, count), 1
    )
    before = jnp.dot(
        jnp.where(chosen, 1.0, 0.0).astype(jnp.bfloat16),
        jnp.where(earlier, 1.0, 0.0).astype(jnp.bfloat16),
        preferred_element_type=jnp.float32,
    )
    place = jnp.where(chosen, before, -1.0)
    row = lax.broadcasted_iota(jnp.int32, (MOST, count), 0).astype(jnp.float32)
    for e in range(experts):
        table_ref[e * MOST : (e + 1) * MOST] = jnp.where(place[e : e + 1] == row, 1.0, 0.0).astype(jnp.bfloat16)
    table = table_ref[...]
    packed = jnp.dot(table, tokens_ref[...], preferred_element_type=jnp.float32)
    packed_ref[:, :width] = packed.astype(jnp.bfloat16)
    blank_ref[...] = jnp.zeros(blank_ref.shape, blank_ref.dtype)
    ones = jnp.ones((count, LANES), jnp.bfloat16)
    packed_ref[:, width:] = jnp.dot(table, ones, preferred_element_type=jnp.float32).astype(jnp.bfloat16)


def pack(tokens, expert_ranks, capacity):
    count, width = tokens.shape
    rows_all = expert_ranks.shape[0] * MOST
    return pl.pallas_call(
        pack_kernel,
        out_shape=[
            jax.ShapeDtypeStruct((rows_all, width + LANES), jnp.bfloat16),
            pltpu.HBM((rows_all, count), jnp.bfloat16),
            pltpu.HBM((rows_all, width), jnp.bfloat16),
        ],
        compiler_params=pltpu.CompilerParams(vmem_limit_bytes=VMEM_LIMIT),
        name="pack",
    )(tokens, expert_ranks, capacity[:, None])


def place_kernel(arrived_ref, step_ref, gates_ref, top_ref, bottom_ref, here_ref):
    rows_all = arrived_ref.shape[0]
    half, width = bottom_ref.shape
    taken = arrived_ref[:, width:]
    earlier = lax.broadcasted_iota(jnp.int32, (rows_all, rows_all), 1) < lax.broadcasted_iota(
        jnp.int32, (rows_all, rows_all), 0
    )
    place = jnp.dot(
        jnp.where(earlier, 1.0, 0.0).astype(jnp.bfloat16), taken, preferred_element_type=jnp.float32
    )
    here = jnp.where(wide(taken) > 0.0, place, -1.0) - (step_ref[0] * 2 * half).astype(jnp.float32)
    here_ref[...] = here
    slots = lax.broadcasted_iota(jnp.int32, (rows_all, 2 * half), 1).astype(jnp.float32)
    table = jnp.where(here[:, :1] == slots, 1.0, 0.0).astype(jnp.bfloat16)
    plane = lax.dot_general(
        table, arrived_ref[:, :width], (((0,), (0,)), ((), ())), preferred_element_type=jnp.float32
    )
    count = place[rows_all - 1 :] + wide(taken[rows_all - 1 :])
    gates = gates_ref.shape[1]
    top_ref[:NOTE] = jnp.zeros((NOTE, width), top_ref.dtype)
    top_ref[:NOTE, :gates] = jnp.broadcast_to(gates_ref[...], (NOTE, gates)).astype(top_ref.dtype)
    top_ref[:NOTE, gates : gates + LANES] = jnp.broadcast_to(count, (NOTE, LANES)).astype(top_ref.dtype)
    top_ref[NOTE:] = plane[:half].astype(top_ref.dtype)
    bottom_ref[...] = plane[half:].astype(bottom_ref.dtype)


def place(arrived, step, gate_pieces, half):
    rows_all = arrived.shape[0]
    width = arrived.shape[1] - LANES
    near = pl.BlockSpec(memory_space=pltpu.VMEM)
    return pl.pallas_call(
        place_kernel,
        in_specs=[near, pl.BlockSpec(memory_space=pltpu.SMEM), near],
        out_shape=[
            jax.ShapeDtypeStruct((NOTE + half, width), jnp.bfloat16),
            jax.ShapeDtypeStruct((half, width), jnp.bfloat16),
            jax.ShapeDtypeStruct((rows_all, LANES), jnp.float32),
        ],
        compiler_params=pltpu.CompilerParams(vmem_limit_bytes=VMEM_LIMIT),
        name="place",
    )(arrived, step, gate_pieces)


def finish_kernel(*refs):
    step_ref, own_ref, *refs, here_ref, kept_ref, out_ref, next_ref, most_ref, scaled_ref = refs
    parts, notes = refs[:6], [note[...].astype(jnp.float32)[:1] for note in refs[6:]]
    half = parts[0].shape[0]
    count = 2 * half
    own, step = own_ref[0], step_ref[0]
    planes = [lax.rem(own + j, len(notes)) for j in range(len(notes))]
    first = jnp.full((1, LANES), (step * count).astype(jnp.float32))
    most = jnp.zeros((1, LANES), jnp.float32)
    for plane, note in zip(planes, notes):
        rows = note[:, 3 * LANES :]
        first = first + jnp.where(plane < own, rows, 0.0)
        most = jnp.maximum(most, rows)
    next_ref[0] = step + 1
    most_ref[0] = jnp.max(most).astype(jnp.int32)
    slots = first + lax.broadcasted_iota(jnp.int32, (count, LANES), 0).astype(jnp.float32)
    lanes = lax.broadcasted_iota(jnp.int32, (1, LANES), 1)
    gates = jnp.zeros((count, LANES), jnp.float32)
    for plane, note in zip(planes, notes):
        gate = note[:, :LANES] + note[:, LANES : 2 * LANES] + note[:, 2 * LANES : 3 * LANES]
        gates = gates + jnp.where(slots == (plane * LANES + lanes).astype(jnp.float32), gate, 0.0)
    gates = jnp.sum(gates, axis=1, keepdims=True)
    for i, (mine, one, other) in enumerate((parts[:3], parts[3:])):
        sums = mine[...] + wide(one[...]) + wide(other[...])
        scaled_ref[i * half : (i + 1) * half] = narrow(gates[i * half : (i + 1) * half] * sums)
    here = here_ref[:, :1]
    places = lax.broadcasted_iota(jnp.int32, (here.shape[0], count), 1).astype(jnp.float32)
    table = jnp.where(here == places, 1.0, 0.0).astype(jnp.bfloat16)
    returned = jnp.dot(table, scaled_ref[...], preferred_element_type=jnp.float32)
    inside = jnp.logical_and(here >= 0.0, here < count)
    out_ref[...] = narrow(jnp.where(inside, returned, wide(kept_ref[...])))


def finish(step, own_dp, parts, notes, here, kept):
    half, width = parts[0].shape
    near, scalar = pl.BlockSpec(memory_space=pltpu.VMEM), pl.BlockSpec(memory_space=pltpu.SMEM)
    corner = pl.BlockSpec((NOTE, 4 * LANES), lambda i: (0, 0))
    return pl.pallas_call(
        finish_kernel,
        grid=(1,),
        in_specs=[scalar] * 2 + [near] * len(parts) + [corner] * len(notes) + [near] * 2,
        out_specs=[near, scalar, scalar],
        out_shape=[
            jax.ShapeDtypeStruct(kept.shape, kept.dtype),
            jax.ShapeDtypeStruct((1,), jnp.int32),
            jax.ShapeDtypeStruct((1,), jnp.int32),
        ],
        scratch_shapes=[pltpu.VMEM((2 * half, width), jnp.bfloat16)],
        compiler_params=pltpu.CompilerParams(vmem_limit_bytes=VMEM_LIMIT),
        name="finish",
    )(step, own_dp, *parts, *notes, here, kept)


def ring_experts(top, bottom, first_weight, second_weight, dp_count):
    far = dp_count // 2
    half = bottom.shape[0]
    upward = [(i, (i + 1) % dp_count) for i in range(dp_count)]
    downward = [(i, (i - 1) % dp_count) for i in range(dp_count)]

    def hop(up_rows, down_rows):
        up_rows = lax.ppermute(up_rows, "dp", upward)
        down_rows = lax.ppermute(down_rows, "dp", downward)
        return up_rows, down_rows

    def mlp(*pieces, sent=(), staged=False):
        kinds = [jnp.bfloat16 if i in sent else jnp.float32 for i in range(len(pieces))]
        return expert_rows(pieces, first_weight, second_weight, half, kinds, staged)

    def after(rows, *others):
        return lax.optimization_barrier((rows, others))[0]

    notes = {0: top}
    firsts = hop(top, bottom)
    seconds = hop(bottom, top)
    outs, done = {}, ()
    for k in range(1, far):
        firsts = after(firsts, *done)
        seconds = after(seconds, *firsts)
        notes[-k % dp_count], notes[k] = firsts[0], seconds[1]
        next_firsts = hop(*firsts)
        if k < far - 1:
            next_seconds = hop(*seconds)
        pieces = firsts[0], seconds[0], seconds[1], firsts[1]
        outs[k] = mlp(*pieces, sent=(0, 3) if k == far - 1 else (), staged=k == 1)
        if k == 1:
            *outs[k], first_weight, second_weight = outs[k]
        done = tuple(outs[k])
        firsts, seconds = next_firsts, next_seconds

    below_top, below_bottom, above_top, above_bottom = outs[far - 1]
    seconds = hop(above_bottom, below_top)
    firsts = after(firsts, above_bottom, below_top, *done)
    notes[far] = firsts[0]
    last = mlp(firsts[0], top, bottom, firsts[1], sent=(0, 3))
    sends = last[0], last[3]
    firsts = hop(*sends)
    for k in range(far - 1, 0, -1):
        if k > 1:
            below_top, _, _, above_bottom = outs[k - 1]
            seconds = after(seconds, *sends)
            sends = narrow(wide(seconds[0]) + above_bottom), narrow(wide(seconds[1]) + below_top)
            seconds = hop(*sends)
        _, below_bottom, above_top, _ = outs[k]
        firsts = after(firsts, *sends)
        sends = narrow(wide(firsts[0]) + above_top), narrow(wide(firsts[1]) + below_bottom)
        firsts = hop(*sends)
    parts = last[1], firsts[0], seconds[1], last[2], seconds[0], firsts[1]
    return parts, [notes[j] for j in range(dp_count)]


def on_device(tokens, expert_ranks, capacity, weight_in, weight_out, gate_weights):
    dp_count = lax.axis_size("dp")
    expert_count = lax.axis_size(EXPERT)
    width = tokens.shape[1]
    slots_dp = gate_weights.shape[1]
    rows_all = expert_count * MOST
    round_rows = slots_dp + slots_dp // 4
    own_dp = lax.axis_index("dp")

    packed, pack_table, blank = pack(tokens, expert_ranks, capacity)
    arrived = lax.all_to_all(
        packed.reshape(expert_count, MOST, width + LANES), EXPERT, split_axis=0, concat_axis=0, tiled=True
    ).reshape(rows_all, width + LANES)
    gate_high = lax.reduce_precision(gate_weights, 8, 7)
    gate_left = gate_weights - gate_high
    gate_middle = lax.reduce_precision(gate_left, 8, 7)
    gate_low = gate_left - gate_middle
    gate_pieces = jnp.concatenate([gate_high, gate_middle, gate_low], axis=1)

    def experts(state):
        step, _, sent_back = state
        top, bottom, here = place(arrived, step, gate_pieces, round_rows // 2)
        parts, notes = ring_experts(top, bottom, weight_in[0], weight_out[0], dp_count)
        sent_back, step, most = finish(step, own_dp.reshape(1), parts, notes, here, sent_back)
        return step, most, sent_back

    _, _, sent_back = lax.while_loop(
        lambda state: state[0][0] * round_rows < state[1][0],
        experts,
        (jnp.zeros((1,), jnp.int32), jnp.ones((1,), jnp.int32), blank),
    )
    results = lax.all_to_all(
        sent_back.reshape(expert_count, MOST, width), EXPERT, split_axis=0, concat_axis=0, tiled=True
    ).reshape(rows_all, width)
    combined = lax.dot_general(
        pack_table, results, (((0,), (0,)), ((), ())), preferred_element_type=jnp.float32
    )
    return combined.astype(jnp.bfloat16)


def solution(mesh):
    split = Mesh(
        mesh.devices.reshape(mesh.shape["dp"], 4, 4, 2), ("dp", "expert_0", "expert_1", "expert_2")
    )
    placed = (
        P(DP_EXPERT, None),
        P(None, DP_EXPERT),
        P(),
        P(EXPERT, None, "dp"),
        P(EXPERT, "dp", None),
        P(EXPERT, "dp"),
    )
    return jax.shard_map(
        on_device, mesh=split, in_specs=placed, out_specs=P(DP_EXPERT, None), check_vma=False
    )
```

```python
import jax
import jax.numpy as jnp
from jax import lax
from jax.experimental import pallas as pl
from jax.experimental.pallas import tpu as pltpu
from jax.sharding import Mesh
from jax.sharding import PartitionSpec as P


MOST = 8
LANES = 128
NOTE = 8
BLOCK = 512
VMEM_LIMIT = 20 * 1024 * 1024
EXPERT = ("expert_0", "expert_1", "expert_2")
DP_EXPERT = ("dp", "expert_0", "expert_1", "expert_2")


def narrow(rows):
    return rows.astype(jnp.bfloat16)


def wide(rows):
    return rows.astype(jnp.float32)


def gather_rows(pieces, rows_ref, half):
    for i, piece in enumerate(pieces):
        rows_ref[i * half : (i + 1) * half] = piece[piece.shape[0] - half :]


def expert_sums(first_ref, second_ref, outs, rows_ref, hidden_ref, first_block, second_block):
    half, width = outs[0].shape

    def hidden_block(i, _):
        block = first_block(i)
        hidden = jnp.dot(rows_ref[...], first_ref[:, block], preferred_element_type=jnp.float32)
        hidden_ref[:, block] = jnp.maximum(hidden, 0.0).astype(jnp.bfloat16)
        return 0

    def out_block(i, _):
        block = second_block(i)
        sums = jnp.dot(hidden_ref[...], second_ref[:, block], preferred_element_type=jnp.float32)
        for j, out in enumerate(outs):
            out[:, block] = sums[j * half : (j + 1) * half].astype(out.dtype)
        return 0

    lax.fori_loop(0, hidden_ref.shape[1] // BLOCK, hidden_block, 0)
    lax.fori_loop(0, width // BLOCK, out_block, 0)


def columns(i):
    return pl.ds(pl.multiple_of(i * BLOCK, BLOCK), BLOCK)


def split_refs(refs):
    count = (len(refs) - 2) // 2
    return refs[:count], refs[count], refs[count + 1], refs[count + 2 :]


def expert_kernel(*refs):
    *refs, rows_ref, hidden_ref = refs
    pieces, first_ref, second_ref, outs = split_refs(refs)
    gather_rows(pieces, rows_ref, outs[0].shape[0])
    expert_sums(first_ref, second_ref, outs, rows_ref, hidden_ref, columns, columns)


def staged_expert_kernel(*refs):
    *refs, first_ref, second_ref, rows_ref, hidden_ref, first_sems, second_sems = refs
    pieces, first_far, second_far, outs = split_refs(refs)

    def first_copy(i):
        return pltpu.make_async_copy(first_far.at[:, columns(i)], first_ref.at[:, columns(i)], first_sems.at[i])

    def second_copy(i):
        return pltpu.make_async_copy(second_far.at[:, columns(i)], second_ref.at[:, columns(i)], second_sems.at[i])

    def first_block(i):
        first_copy(i).wait()
        return columns(i)

    def second_block(i):
        second_copy(i).wait()
        return columns(i)

    for i in range(first_ref.shape[1] // BLOCK):
        first_copy(i).start()
    for i in range(second_ref.shape[1] // BLOCK):
        second_copy(i).start()
    gather_rows(pieces, rows_ref, outs[0].shape[0])
    expert_sums(first_ref, second_ref, outs, rows_ref, hidden_ref, first_block, second_block)


def expert_rows(pieces, first_weight, second_weight, half, kinds, staged):
    width, hidden = first_weight.shape
    count = len(pieces) * half
    scratch = [pltpu.VMEM((count, width), jnp.bfloat16), pltpu.VMEM((count, hidden), jnp.bfloat16)]
    out_shape = [jax.ShapeDtypeStruct((half, width), kind) for kind in kinds]
    specs = {}
    if staged:
        scratch += [
            pltpu.SemaphoreType.DMA((hidden // BLOCK,)),
            pltpu.SemaphoreType.DMA((width // BLOCK,)),
        ]
        out_shape += [pltpu.VMEM(w.shape, w.dtype) for w in (first_weight, second_weight)]
        near, far = pl.BlockSpec(memory_space=pltpu.VMEM), pl.BlockSpec(memory_space=pl.ANY)
        specs = {"in_specs": [near] * len(pieces) + [far] * 2, "out_specs": [near] * len(out_shape)}
    return pl.pallas_call(
        staged_expert_kernel if staged else expert_kernel,
        out_shape=out_shape,
        scratch_shapes=scratch,
        compiler_params=pltpu.CompilerParams(vmem_limit_bytes=VMEM_LIMIT),
        cost_estimate=pl.CostEstimate(
            flops=4 * count * width * hidden,
            transcendentals=0,
            bytes_accessed=4 * width * hidden + 6 * count * width,
        ),
        name="expert_rows",
        **specs,
    )(*pieces, first_weight, second_weight)


def pack_kernel(tokens_ref, ranks_ref, capacity_ref, packed_ref, table_ref, blank_ref):
    experts, count = ranks_ref.shape
    width = tokens_ref.shape[1]
    square = (experts, experts)
    diagonal = lax.broadcasted_iota(jnp.int32, square, 0) == lax.broadcasted_iota(jnp.int32, square, 1)
    limits = jnp.broadcast_to(capacity_ref[...].astype(jnp.float32), square)
    limits = jnp.sum(jnp.where(diagonal, limits, 0.0), axis=1, keepdims=True)
    chosen = ranks_ref[...].astype(jnp.float32) < limits
    earlier = lax.broadcasted_iota(jnp.int32, (count, count), 0) < lax.broadcasted_iota(
        jnp.int32, (count, count), 1
    )
    before = jnp.dot(
        jnp.where(chosen, 1.0, 0.0).astype(jnp.bfloat16),
        jnp.where(earlier, 1.0, 0.0).astype(jnp.bfloat16),
        preferred_element_type=jnp.float32,
    )
    place = jnp.where(chosen, before, -1.0)
    row = lax.broadcasted_iota(jnp.int32, (MOST, count), 0).astype(jnp.float32)
    for e in range(experts):
        table_ref[e * MOST : (e + 1) * MOST] = jnp.where(place[e : e + 1] == row, 1.0, 0.0).astype(jnp.bfloat16)
    table = table_ref[...]
    packed = jnp.dot(table, tokens_ref[...], preferred_element_type=jnp.float32)
    packed_ref[:, :width] = packed.astype(jnp.bfloat16)
    blank_ref[...] = jnp.zeros(blank_ref.shape, blank_ref.dtype)
    ones = jnp.ones((count, LANES), jnp.bfloat16)
    packed_ref[:, width:] = jnp.dot(table, ones, preferred_element_type=jnp.float32).astype(jnp.bfloat16)


def pack(tokens, expert_ranks, capacity):
    count, width = tokens.shape
    rows_all = expert_ranks.shape[0] * MOST
    return pl.pallas_call(
        pack_kernel,
        out_shape=[
            jax.ShapeDtypeStruct((rows_all, width + LANES), jnp.bfloat16),
            pltpu.HBM((rows_all, count), jnp.bfloat16),
            pltpu.HBM((rows_all, width), jnp.bfloat16),
        ],
        compiler_params=pltpu.CompilerParams(vmem_limit_bytes=VMEM_LIMIT),
        name="pack",
    )(tokens, expert_ranks, capacity[None, :])


def place_kernel(arrived_ref, step_ref, gates_ref, top_ref, bottom_ref, here_ref):
    rows_all = arrived_ref.shape[0]
    half, width = bottom_ref.shape
    taken = arrived_ref[:, width:]
    earlier = lax.broadcasted_iota(jnp.int32, (rows_all, rows_all), 1) < lax.broadcasted_iota(
        jnp.int32, (rows_all, rows_all), 0
    )
    place = jnp.dot(
        jnp.where(earlier, 1.0, 0.0).astype(jnp.bfloat16), taken, preferred_element_type=jnp.float32
    )
    here = jnp.where(wide(taken) > 0.0, place, -1.0) - (step_ref[0] * 2 * half).astype(jnp.float32)
    here_ref[...] = here
    slots = lax.broadcasted_iota(jnp.int32, (rows_all, 2 * half), 1).astype(jnp.float32)
    table = jnp.where(here[:, :1] == slots, 1.0, 0.0).astype(jnp.bfloat16)
    plane = lax.dot_general(
        table, arrived_ref[:, :width], (((0,), (0,)), ((), ())), preferred_element_type=jnp.float32
    )
    count = place[rows_all - 1 :] + wide(taken[rows_all - 1 :])
    gates = gates_ref.shape[1]
    top_ref[:NOTE] = jnp.zeros((NOTE, width), top_ref.dtype)
    top_ref[:NOTE, :gates] = jnp.broadcast_to(gates_ref[...], (NOTE, gates)).astype(top_ref.dtype)
    top_ref[:NOTE, gates : gates + LANES] = jnp.broadcast_to(count, (NOTE, LANES)).astype(top_ref.dtype)
    top_ref[NOTE:] = plane[:half].astype(top_ref.dtype)
    bottom_ref[...] = plane[half:].astype(bottom_ref.dtype)


def place(arrived, step, gate_pieces, half):
    rows_all = arrived.shape[0]
    width = arrived.shape[1] - LANES
    near = pl.BlockSpec(memory_space=pltpu.VMEM)
    return pl.pallas_call(
        place_kernel,
        in_specs=[near, pl.BlockSpec(memory_space=pltpu.SMEM), near],
        out_shape=[
            jax.ShapeDtypeStruct((NOTE + half, width), jnp.bfloat16),
            jax.ShapeDtypeStruct((half, width), jnp.bfloat16),
            jax.ShapeDtypeStruct((rows_all, LANES), jnp.float32),
        ],
        compiler_params=pltpu.CompilerParams(vmem_limit_bytes=VMEM_LIMIT),
        name="place",
    )(arrived, step, gate_pieces)


def finish_kernel(*refs):
    step_ref, own_ref, *refs, here_ref, kept_ref, out_ref, next_ref, most_ref, scaled_ref = refs
    parts, notes = refs[:6], [note[...].astype(jnp.float32)[:1] for note in refs[6:]]
    half = parts[0].shape[0]
    count = 2 * half
    own, step = own_ref[0], step_ref[0]
    planes = [lax.rem(own + j, len(notes)) for j in range(len(notes))]
    first = jnp.full((1, LANES), (step * count).astype(jnp.float32))
    most = jnp.zeros((1, LANES), jnp.float32)
    for plane, note in zip(planes, notes):
        rows = note[:, 3 * LANES :]
        first = first + jnp.where(plane < own, rows, 0.0)
        most = jnp.maximum(most, rows)
    next_ref[0] = step + 1
    most_ref[0] = jnp.max(most).astype(jnp.int32)
    slots = first + lax.broadcasted_iota(jnp.int32, (count, LANES), 0).astype(jnp.float32)
    lanes = lax.broadcasted_iota(jnp.int32, (1, LANES), 1)
    gates = jnp.zeros((count, LANES), jnp.float32)
    for plane, note in zip(planes, notes):
        gate = note[:, :LANES] + note[:, LANES : 2 * LANES] + note[:, 2 * LANES : 3 * LANES]
        gates = gates + jnp.where(slots == (plane * LANES + lanes).astype(jnp.float32), gate, 0.0)
    gates = jnp.sum(gates, axis=1, keepdims=True)
    for i, (mine, one, other) in enumerate((parts[:3], parts[3:])):
        sums = mine[...] + wide(one[...]) + wide(other[...])
        scaled_ref[i * half : (i + 1) * half] = narrow(gates[i * half : (i + 1) * half] * sums)
    here = here_ref[:, :1]
    places = lax.broadcasted_iota(jnp.int32, (here.shape[0], count), 1).astype(jnp.float32)
    table = jnp.where(here == places, 1.0, 0.0).astype(jnp.bfloat16)
    returned = jnp.dot(table, scaled_ref[...], preferred_element_type=jnp.float32)
    inside = jnp.logical_and(here >= 0.0, here < count)
    out_ref[...] = narrow(jnp.where(inside, returned, wide(kept_ref[...])))


def finish(step, own_dp, parts, notes, here, kept):
    half, width = parts[0].shape
    near, scalar = pl.BlockSpec(memory_space=pltpu.VMEM), pl.BlockSpec(memory_space=pltpu.SMEM)
    corner = pl.BlockSpec((NOTE, 4 * LANES), lambda i: (0, 0))
    return pl.pallas_call(
        finish_kernel,
        grid=(1,),
        in_specs=[scalar] * 2 + [near] * len(parts) + [corner] * len(notes) + [near] * 2,
        out_specs=[near, scalar, scalar],
        out_shape=[
            jax.ShapeDtypeStruct(kept.shape, kept.dtype),
            jax.ShapeDtypeStruct((1,), jnp.int32),
            jax.ShapeDtypeStruct((1,), jnp.int32),
        ],
        scratch_shapes=[pltpu.VMEM((2 * half, width), jnp.bfloat16)],
        compiler_params=pltpu.CompilerParams(vmem_limit_bytes=VMEM_LIMIT),
        name="finish",
    )(step, own_dp, *parts, *notes, here, kept)


def ring_experts(top, bottom, first_weight, second_weight, dp_count):
    far = dp_count // 2
    half = bottom.shape[0]
    upward = [(i, (i + 1) % dp_count) for i in range(dp_count)]
    downward = [(i, (i - 1) % dp_count) for i in range(dp_count)]

    def hop(up_rows, down_rows):
        up_rows = lax.ppermute(up_rows, "dp", upward)
        down_rows = lax.ppermute(down_rows, "dp", downward)
        return up_rows, down_rows

    def mlp(*pieces, sent=(), staged=False):
        kinds = [jnp.bfloat16 if i in sent else jnp.float32 for i in range(len(pieces))]
        return expert_rows(pieces, first_weight, second_weight, half, kinds, staged)

    def after(rows, *others):
        return lax.optimization_barrier((rows, others))[0]

    notes = {0: top}
    firsts = hop(top, bottom)
    seconds = hop(bottom, top)
    *own, first_weight, second_weight = mlp(top, bottom, staged=True)
    below, above, done = {}, {}, own
    for k in range(1, far):
        firsts = after(firsts, *done)
        seconds = after(seconds, *firsts)
        notes[-k % dp_count], notes[k] = firsts[0], seconds[1]
        next_firsts = hop(*firsts)
        if k < far - 1:
            next_seconds = hop(*seconds)
            done = mlp(firsts[0], seconds[0], seconds[1], firsts[1])
            below[k], above[k] = done[:2], done[2:]
            seconds = next_seconds
        else:
            below_top, above_bottom = mlp(*firsts, sent=(0, 1))
            seconds_back = hop(above_bottom, below_top)
            seconds = after(seconds, above_bottom, below_top)
            below_bottom, above_top = mlp(*seconds)
            below[k], above[k] = (below_top, below_bottom), (above_top, above_bottom)
        firsts = next_firsts

    firsts = after(firsts, below_bottom, above_top)
    notes[far] = firsts[0]
    sends = tuple(mlp(*firsts, sent=(0, 1)))
    seconds = seconds_back
    firsts = hop(*sends)
    for k in range(far - 1, 0, -1):
        if k > 1:
            seconds = after(seconds, *sends)
            sends = narrow(wide(seconds[0]) + above[k - 1][1]), narrow(wide(seconds[1]) + below[k - 1][0])
            seconds = hop(*sends)
        firsts = after(firsts, *sends)
        sends = narrow(wide(firsts[0]) + above[k][0]), narrow(wide(firsts[1]) + below[k][1])
        firsts = hop(*sends)
    parts = own[0], firsts[0], seconds[1], own[1], seconds[0], firsts[1]
    return parts, [notes[j] for j in range(dp_count)]


def on_device(tokens, expert_ranks, capacity, weight_in, weight_out, gate_weights):
    dp_count = lax.axis_size("dp")
    expert_count = lax.axis_size(EXPERT)
    width = tokens.shape[1]
    slots_dp = gate_weights.shape[1]
    rows_all = expert_count * MOST
    round_rows = slots_dp + slots_dp // 4
    own_dp = lax.axis_index("dp")

    packed, pack_table, blank = pack(tokens, expert_ranks, capacity)
    arrived = lax.all_to_all(
        packed.reshape(expert_count, MOST, width + LANES), EXPERT, split_axis=0, concat_axis=0, tiled=True
    ).reshape(rows_all, width + LANES)
    gate_high = lax.reduce_precision(gate_weights, 8, 7)
    gate_left = gate_weights - gate_high
    gate_middle = lax.reduce_precision(gate_left, 8, 7)
    gate_low = gate_left - gate_middle
    gate_pieces = jnp.concatenate([gate_high, gate_middle, gate_low], axis=1)

    def experts(state):
        step, _, sent_back = state
        top, bottom, here = place(arrived, step, gate_pieces, round_rows // 2)
        parts, notes = ring_experts(top, bottom, weight_in[0], weight_out[0], dp_count)
        sent_back, step, most = finish(step, own_dp.reshape(1), parts, notes, here, sent_back)
        return step, most, sent_back

    _, _, sent_back = lax.while_loop(
        lambda state: state[0][0] * round_rows < state[1][0],
        experts,
        (jnp.zeros((1,), jnp.int32), jnp.ones((1,), jnp.int32), blank),
    )
    results = lax.all_to_all(
        sent_back.reshape(expert_count, MOST, width), EXPERT, split_axis=0, concat_axis=0, tiled=True
    ).reshape(rows_all, width)
    combined = lax.dot_general(
        pack_table, results, (((0,), (0,)), ((), ())), preferred_element_type=jnp.float32
    )
    return combined.astype(jnp.bfloat16)


def solution(mesh):
    split = Mesh(
        mesh.devices.reshape(mesh.shape["dp"], 4, 4, 2), ("dp", "expert_0", "expert_1", "expert_2")
    )
    placed = (
        P(DP_EXPERT, None),
        P(None, DP_EXPERT),
        P(),
        P(EXPERT, None, "dp"),
        P(EXPERT, "dp", None),
        P(EXPERT, "dp"),
    )
    return jax.shard_map(
        on_device, mesh=split, in_specs=placed, out_specs=P(DP_EXPERT, None), check_vma=False
    )
```

```python
import jax
import jax.numpy as jnp
from jax import lax
from jax.experimental import pallas as pl
from jax.experimental.pallas import tpu as pltpu
from jax.sharding import Mesh
from jax.sharding import PartitionSpec as P


MOST = 8
LANES = 128
NOTE = 8
BLOCK = 512
VMEM_LIMIT = 20 * 1024 * 1024
EXPERT = ("expert_0", "expert_1", "expert_2")
DP_EXPERT = ("dp", "expert_0", "expert_1", "expert_2")


def narrow(rows):
    return rows.astype(jnp.bfloat16)


def wide(rows):
    return rows.astype(jnp.float32)


def gather_rows(pieces, rows_ref, half):
    for i, piece in enumerate(pieces):
        rows_ref[i * half : (i + 1) * half] = piece[piece.shape[0] - half :]


def expert_sums(first_ref, second_ref, outs, rows_ref, hidden_ref, first_block, second_block):
    half, width = outs[0].shape

    def hidden_block(i, _):
        block = first_block(i)
        hidden = jnp.dot(rows_ref[...], first_ref[:, block], preferred_element_type=jnp.float32)
        hidden_ref[:, block] = jnp.maximum(hidden, 0.0).astype(jnp.bfloat16)
        return 0

    def out_block(i, _):
        block = second_block(i)
        sums = jnp.dot(hidden_ref[...], second_ref[:, block], preferred_element_type=jnp.float32)
        for j, out in enumerate(outs):
            out[:, block] = sums[j * half : (j + 1) * half].astype(out.dtype)
        return 0

    lax.fori_loop(0, hidden_ref.shape[1] // BLOCK, hidden_block, 0)
    lax.fori_loop(0, width // BLOCK, out_block, 0)


def columns(i):
    return pl.ds(pl.multiple_of(i * BLOCK, BLOCK), BLOCK)


def split_refs(refs):
    count = (len(refs) - 2) // 2
    return refs[:count], refs[count], refs[count + 1], refs[count + 2 :]


def expert_kernel(*refs):
    *refs, rows_ref, hidden_ref = refs
    pieces, first_ref, second_ref, outs = split_refs(refs)
    gather_rows(pieces, rows_ref, outs[0].shape[0])
    expert_sums(first_ref, second_ref, outs, rows_ref, hidden_ref, columns, columns)


def staged_expert_kernel(*refs):
    *refs, first_ref, second_ref, rows_ref, hidden_ref, first_sems, second_sems = refs
    pieces, first_far, second_far, outs = split_refs(refs)

    def first_copy(i):
        return pltpu.make_async_copy(first_far.at[:, columns(i)], first_ref.at[:, columns(i)], first_sems.at[i])

    def second_copy(i):
        return pltpu.make_async_copy(second_far.at[:, columns(i)], second_ref.at[:, columns(i)], second_sems.at[i])

    def first_block(i):
        first_copy(i).wait()
        return columns(i)

    def second_block(i):
        second_copy(i).wait()
        return columns(i)

    for i in range(first_ref.shape[1] // BLOCK):
        first_copy(i).start()
    for i in range(second_ref.shape[1] // BLOCK):
        second_copy(i).start()
    gather_rows(pieces, rows_ref, outs[0].shape[0])
    expert_sums(first_ref, second_ref, outs, rows_ref, hidden_ref, first_block, second_block)


def expert_rows(pieces, first_weight, second_weight, half, kinds, staged):
    width, hidden = first_weight.shape
    count = len(pieces) * half
    scratch = [pltpu.VMEM((count, width), jnp.bfloat16), pltpu.VMEM((count, hidden), jnp.bfloat16)]
    out_shape = [jax.ShapeDtypeStruct((half, width), kind) for kind in kinds]
    specs = {}
    if staged:
        scratch += [
            pltpu.SemaphoreType.DMA((hidden // BLOCK,)),
            pltpu.SemaphoreType.DMA((width // BLOCK,)),
        ]
        out_shape += [pltpu.VMEM(w.shape, w.dtype) for w in (first_weight, second_weight)]
        near, far = pl.BlockSpec(memory_space=pltpu.VMEM), pl.BlockSpec(memory_space=pl.ANY)
        specs = {"in_specs": [near] * len(pieces) + [far] * 2, "out_specs": [near] * len(out_shape)}
    return pl.pallas_call(
        staged_expert_kernel if staged else expert_kernel,
        out_shape=out_shape,
        scratch_shapes=scratch,
        compiler_params=pltpu.CompilerParams(vmem_limit_bytes=VMEM_LIMIT),
        cost_estimate=pl.CostEstimate(
            flops=4 * count * width * hidden,
            transcendentals=0,
            bytes_accessed=4 * width * hidden + 6 * count * width,
        ),
        name="expert_rows",
        **specs,
    )(*pieces, first_weight, second_weight)


def pack_kernel(tokens_ref, ranks_ref, capacity_ref, packed_ref, table_ref, blank_ref):
    experts, count = ranks_ref.shape
    width = tokens_ref.shape[1]
    square = (experts, experts)
    diagonal = lax.broadcasted_iota(jnp.int32, square, 0) == lax.broadcasted_iota(jnp.int32, square, 1)
    limits = jnp.broadcast_to(capacity_ref[...].astype(jnp.float32), square)
    limits = jnp.sum(jnp.where(diagonal, limits, 0.0), axis=1, keepdims=True)
    chosen = ranks_ref[...].astype(jnp.float32) < limits
    earlier = lax.broadcasted_iota(jnp.int32, (count, count), 0) < lax.broadcasted_iota(
        jnp.int32, (count, count), 1
    )
    before = jnp.dot(
        jnp.where(chosen, 1.0, 0.0).astype(jnp.bfloat16),
        jnp.where(earlier, 1.0, 0.0).astype(jnp.bfloat16),
        preferred_element_type=jnp.float32,
    )
    place = jnp.where(chosen, before, -1.0)
    row = lax.broadcasted_iota(jnp.int32, (MOST, count), 0).astype(jnp.float32)
    for e in range(experts):
        table_ref[e * MOST : (e + 1) * MOST] = jnp.where(place[e : e + 1] == row, 1.0, 0.0).astype(jnp.bfloat16)
    table = table_ref[...]
    packed = jnp.dot(table, tokens_ref[...], preferred_element_type=jnp.float32)
    packed_ref[:, :width] = packed.astype(jnp.bfloat16)
    blank_ref[...] = jnp.zeros(blank_ref.shape, blank_ref.dtype)
    ones = jnp.ones((count, LANES), jnp.bfloat16)
    packed_ref[:, width:] = jnp.dot(table, ones, preferred_element_type=jnp.float32).astype(jnp.bfloat16)


def pack(tokens, expert_ranks, capacity):
    count, width = tokens.shape
    rows_all = expert_ranks.shape[0] * MOST
    return pl.pallas_call(
        pack_kernel,
        out_shape=[
            jax.ShapeDtypeStruct((rows_all, width + LANES), jnp.bfloat16),
            pltpu.HBM((rows_all, count), jnp.bfloat16),
            pltpu.HBM((rows_all, width), jnp.bfloat16),
        ],
        compiler_params=pltpu.CompilerParams(vmem_limit_bytes=VMEM_LIMIT),
        name="pack",
    )(tokens, expert_ranks, capacity[None, :])


def place_kernel(arrived_ref, step_ref, gates_ref, top_ref, bottom_ref, here_ref):
    rows_all = arrived_ref.shape[0]
    half, width = bottom_ref.shape
    taken = arrived_ref[:, width:]
    earlier = lax.broadcasted_iota(jnp.int32, (rows_all, rows_all), 1) < lax.broadcasted_iota(
        jnp.int32, (rows_all, rows_all), 0
    )
    place = jnp.dot(
        jnp.where(earlier, 1.0, 0.0).astype(jnp.bfloat16), taken, preferred_element_type=jnp.float32
    )
    here = jnp.where(wide(taken) > 0.0, place, -1.0) - (step_ref[0] * (2 * half - 1)).astype(jnp.float32)
    here_ref[...] = here
    slots = lax.broadcasted_iota(jnp.int32, (rows_all, 2 * half), 1).astype(jnp.float32)
    table = jnp.where(here[:, :1] + 1.0 == slots, 1.0, 0.0).astype(jnp.bfloat16)
    plane = lax.dot_general(
        table, arrived_ref[:, :width], (((0,), (0,)), ((), ())), preferred_element_type=jnp.float32
    )
    count = place[rows_all - 1 :] + wide(taken[rows_all - 1 :])
    blank = jnp.zeros((1, width - gates_ref.shape[1] - LANES), jnp.float32)
    note = jnp.concatenate([gates_ref[...], count, blank], axis=1)
    row = lax.broadcasted_iota(jnp.int32, (half, width), 0)
    top_ref[...] = jnp.where(row == 0, jnp.broadcast_to(note, (half, width)), plane[:half]).astype(top_ref.dtype)
    bottom_ref[...] = plane[half:].astype(bottom_ref.dtype)


def place(arrived, step, gate_pieces, half):
    rows_all = arrived.shape[0]
    width = arrived.shape[1] - LANES
    near = pl.BlockSpec(memory_space=pltpu.VMEM)
    return pl.pallas_call(
        place_kernel,
        in_specs=[near, pl.BlockSpec(memory_space=pltpu.SMEM), near],
        out_shape=[
            jax.ShapeDtypeStruct((half, width), jnp.bfloat16),
            jax.ShapeDtypeStruct((half, width), jnp.bfloat16),
            jax.ShapeDtypeStruct((rows_all, LANES), jnp.float32),
        ],
        compiler_params=pltpu.CompilerParams(vmem_limit_bytes=VMEM_LIMIT),
        name="place",
    )(arrived, step, gate_pieces)


def finish_kernel(*refs):
    step_ref, own_ref, *refs, here_ref, kept_ref, out_ref, next_ref, most_ref, scaled_ref = refs
    parts, notes = refs[:8], [note[...].astype(jnp.float32)[:1] for note in refs[8:]]
    half = parts[0].shape[0]
    count = 2 * half
    own, step = own_ref[0], step_ref[0]
    planes = [lax.rem(own + j, len(notes)) for j in range(len(notes))]
    first = jnp.full((1, LANES), (step * (count - 1) - 1).astype(jnp.float32))
    most = jnp.zeros((1, LANES), jnp.float32)
    for plane, note in zip(planes, notes):
        rows = note[:, 3 * LANES :]
        first = first + jnp.where(plane < own, rows, 0.0)
        most = jnp.maximum(most, rows)
    next_ref[0] = step + 1
    most_ref[0] = jnp.max(most).astype(jnp.int32)
    slots = first + lax.broadcasted_iota(jnp.int32, (count, LANES), 0).astype(jnp.float32)
    lanes = lax.broadcasted_iota(jnp.int32, (1, LANES), 1)
    gates = jnp.zeros((count, LANES), jnp.float32)
    for plane, note in zip(planes, notes):
        gate = note[:, :LANES] + note[:, LANES : 2 * LANES] + note[:, 2 * LANES : 3 * LANES]
        gates = gates + jnp.where(slots == (plane * LANES + lanes).astype(jnp.float32), gate, 0.0)
    gates = jnp.sum(gates, axis=1, keepdims=True)
    quarter = half // 2
    for i, (mine, near, *fars) in enumerate((parts[:4], parts[4:])):
        for j, far in enumerate(fars):
            rows = slice(j * quarter, (j + 1) * quarter)
            sums = mine[rows] + wide(near[rows]) + wide(far[...])
            part = slice(i * half + j * quarter, i * half + (j + 1) * quarter)
            scaled_ref[part] = narrow(gates[part] * sums)
    here = here_ref[:, :1]
    places = lax.broadcasted_iota(jnp.int32, (here.shape[0], count), 1).astype(jnp.float32)
    table = jnp.where(here + 1.0 == places, 1.0, 0.0).astype(jnp.bfloat16)
    returned = jnp.dot(table, scaled_ref[...], preferred_element_type=jnp.float32)
    inside = jnp.logical_and(here >= 0.0, here < count - 1)
    out_ref[...] = narrow(jnp.where(inside, returned, wide(kept_ref[...])))


def finish(step, own_dp, parts, notes, here, kept):
    half, width = parts[0].shape
    near, scalar = pl.BlockSpec(memory_space=pltpu.VMEM), pl.BlockSpec(memory_space=pltpu.SMEM)
    corner = pl.BlockSpec((NOTE, 4 * LANES), lambda i: (0, 0))
    return pl.pallas_call(
        finish_kernel,
        grid=(1,),
        in_specs=[scalar] * 2 + [near] * len(parts) + [corner] * len(notes) + [near] * 2,
        out_specs=[near, scalar, scalar],
        out_shape=[
            jax.ShapeDtypeStruct(kept.shape, kept.dtype),
            jax.ShapeDtypeStruct((1,), jnp.int32),
            jax.ShapeDtypeStruct((1,), jnp.int32),
        ],
        scratch_shapes=[pltpu.VMEM((2 * half, width), jnp.bfloat16)],
        compiler_params=pltpu.CompilerParams(vmem_limit_bytes=VMEM_LIMIT),
        name="finish",
    )(step, own_dp, *parts, *notes, here, kept)


def ring_experts(top, bottom, first_weight, second_weight, dp_count):
    far = dp_count // 2
    half = bottom.shape[0]
    upward = [(i, (i + 1) % dp_count) for i in range(dp_count)]
    downward = [(i, (i - 1) % dp_count) for i in range(dp_count)]

    def hop(up_rows, down_rows):
        up_rows = lax.ppermute(up_rows, "dp", upward)
        down_rows = lax.ppermute(down_rows, "dp", downward)
        return up_rows, down_rows

    def mlp(*pieces, sent=(), staged=False):
        kinds = [jnp.bfloat16 if i in sent else jnp.float32 for i in range(len(pieces))]
        return expert_rows(pieces, first_weight, second_weight, half, kinds, staged)

    def after(rows, *others):
        return lax.optimization_barrier((rows, others))[0]

    notes = {0: top}
    firsts = hop(top, bottom)
    seconds = hop(bottom, top)
    *own, first_weight, second_weight = mlp(top, bottom, staged=True)
    below, above, done = {}, {}, own
    for k in range(1, far):
        firsts = after(firsts, *done)
        seconds = after(seconds, *firsts)
        notes[-k % dp_count], notes[k] = firsts[0], seconds[1]
        next_firsts = hop(*firsts)
        if k < far - 1:
            next_seconds = hop(*seconds)
            done = mlp(firsts[0], seconds[0], seconds[1], firsts[1])
            below[k], above[k] = done[:2], done[2:]
            seconds = next_seconds
        else:
            below_top, above_bottom = mlp(*firsts, sent=(0, 1))
            seconds_back = hop(above_bottom, below_top)
            seconds = after(seconds, above_bottom, below_top)
            below_bottom, above_top = mlp(*seconds)
            below[k], above[k] = (below_top, below_bottom), (above_top, above_bottom)
        firsts = next_firsts

    firsts = after(firsts, below_bottom, above_top)
    notes[far] = firsts[0]
    sends = tuple(mlp(*firsts, sent=(0, 1)))
    seconds = seconds_back
    firsts = hop(*sends)
    for k in range(far - 1, 1, -1):
        seconds = after(seconds, *sends)
        sends = narrow(wide(seconds[0]) + above[k - 1][1]), narrow(wide(seconds[1]) + below[k - 1][0])
        seconds = hop(*sends)
        firsts = after(firsts, *sends)
        if k > 2:
            sends = narrow(wide(firsts[0]) + above[k][0]), narrow(wide(firsts[1]) + below[k][1])
            firsts = hop(*sends)
    quarters = [slice(0, half // 2), slice(half // 2, half)]
    hops = []
    for part in quarters:
        sends = narrow(wide(firsts[0][part]) + above[2][0][part]), narrow(wide(firsts[1][part]) + below[2][1][part])
        hops.append(hop(*sends))
    fars = []
    for j, part in enumerate(quarters):
        firsts = after(hops[j], *sends)
        sends = narrow(wide(firsts[0]) + above[1][0][part]), narrow(wide(firsts[1]) + below[1][1][part])
        fars.append(hop(*sends))
    parts = own[0], seconds[1], fars[0][0], fars[1][0], own[1], seconds[0], fars[0][1], fars[1][1]
    return parts, [notes[j] for j in range(dp_count)]


def on_device(tokens, expert_ranks, capacity, weight_in, weight_out, gate_weights):
    dp_count = lax.axis_size("dp")
    expert_count = lax.axis_size(EXPERT)
    width = tokens.shape[1]
    slots_dp = gate_weights.shape[1]
    rows_all = expert_count * MOST
    half = (slots_dp + slots_dp // 4) // 2
    round_rows = 2 * half - 1
    own_dp = lax.axis_index("dp")

    packed, pack_table, blank = pack(tokens, expert_ranks, capacity)
    arrived = lax.all_to_all(
        packed.reshape(expert_count, MOST, width + LANES), EXPERT, split_axis=0, concat_axis=0, tiled=True
    ).reshape(rows_all, width + LANES)
    gate_high = lax.reduce_precision(gate_weights, 8, 7)
    gate_left = gate_weights - gate_high
    gate_middle = lax.reduce_precision(gate_left, 8, 7)
    gate_low = gate_left - gate_middle
    gate_pieces = jnp.concatenate([gate_high, gate_middle, gate_low], axis=1)

    def experts(state):
        step, _, sent_back = state
        top, bottom, here = place(arrived, step, gate_pieces, half)
        parts, notes = ring_experts(top, bottom, weight_in[0], weight_out[0], dp_count)
        sent_back, step, most = finish(step, own_dp.reshape(1), parts, notes, here, sent_back)
        return step, most, sent_back

    _, _, sent_back = lax.while_loop(
        lambda state: state[0][0] * round_rows < state[1][0],
        experts,
        (jnp.zeros((1,), jnp.int32), jnp.ones((1,), jnp.int32), blank),
    )
    results = lax.all_to_all(
        sent_back.reshape(expert_count, MOST, width), EXPERT, split_axis=0, concat_axis=0, tiled=True
    ).reshape(rows_all, width)
    combined = lax.dot_general(
        pack_table, results, (((0,), (0,)), ((), ())), preferred_element_type=jnp.float32
    )
    return combined.astype(jnp.bfloat16)


def solution(mesh):
    split = Mesh(
        mesh.devices.reshape(mesh.shape["dp"], 4, 4, 2), ("dp", "expert_0", "expert_1", "expert_2")
    )
    placed = (
        P(DP_EXPERT, None),
        P(None, DP_EXPERT),
        P(),
        P(EXPERT, None, "dp"),
        P(EXPERT, "dp", None),
        P(EXPERT, "dp"),
    )
    return jax.shard_map(
        on_device, mesh=split, in_specs=placed, out_specs=P(DP_EXPERT, None), check_vma=False
    )
```

```python
import jax
import jax.numpy as jnp
from jax import lax
from jax.experimental import pallas as pl
from jax.experimental.pallas import tpu as pltpu
from jax.sharding import Mesh
from jax.sharding import PartitionSpec as P


MOST = 8
LANES = 128
NOTE = 8
BLOCK = 512
VMEM_LIMIT = 20 * 1024 * 1024
PACK_LIMIT = 60 * 1024 * 1024
EXPERT = ("expert_0", "expert_1", "expert_2")
DP_EXPERT = ("dp", "expert_0", "expert_1", "expert_2")


def narrow(rows):
    return rows.astype(jnp.bfloat16)


def wide(rows):
    return rows.astype(jnp.float32)


def gather_rows(pieces, rows_ref, half):
    for i, piece in enumerate(pieces):
        rows_ref[i * half : (i + 1) * half] = piece[piece.shape[0] - half :]


def expert_sums(first_ref, second_ref, outs, rows_ref, hidden_ref, first_block, second_block):
    half, width = outs[0].shape

    def hidden_block(i, _):
        block = first_block(i)
        hidden = jnp.dot(rows_ref[...], first_ref[:, block], preferred_element_type=jnp.float32)
        hidden_ref[:, block] = jnp.maximum(hidden, 0.0).astype(jnp.bfloat16)
        return 0

    def out_block(i, _):
        block = second_block(i)
        sums = jnp.dot(hidden_ref[...], second_ref[:, block], preferred_element_type=jnp.float32)
        for j, out in enumerate(outs):
            out[:, block] = sums[j * half : (j + 1) * half].astype(out.dtype)
        return 0

    lax.fori_loop(0, hidden_ref.shape[1] // BLOCK, hidden_block, 0)
    lax.fori_loop(0, width // BLOCK, out_block, 0)


def columns(i):
    return pl.ds(pl.multiple_of(i * BLOCK, BLOCK), BLOCK)


def split_refs(refs):
    count = (len(refs) - 2) // 2
    return refs[:count], refs[count], refs[count + 1], refs[count + 2 :]


def expert_kernel(*refs):
    *refs, rows_ref, hidden_ref = refs
    pieces, first_ref, second_ref, outs = split_refs(refs)
    gather_rows(pieces, rows_ref, outs[0].shape[0])
    expert_sums(first_ref, second_ref, outs, rows_ref, hidden_ref, columns, columns)


def staged_expert_kernel(*refs):
    *refs, first_ref, second_ref, rows_ref, hidden_ref, first_sems, second_sems = refs
    pieces, first_far, second_far, outs = split_refs(refs)

    def first_copy(i):
        return pltpu.make_async_copy(first_far.at[:, columns(i)], first_ref.at[:, columns(i)], first_sems.at[i])

    def second_copy(i):
        return pltpu.make_async_copy(second_far.at[:, columns(i)], second_ref.at[:, columns(i)], second_sems.at[i])

    def first_block(i):
        first_copy(i).wait()
        return columns(i)

    def second_block(i):
        second_copy(i).wait()
        return columns(i)

    for i in range(first_ref.shape[1] // BLOCK):
        first_copy(i).start()
    for i in range(second_ref.shape[1] // BLOCK):
        second_copy(i).start()
    gather_rows(pieces, rows_ref, outs[0].shape[0])
    expert_sums(first_ref, second_ref, outs, rows_ref, hidden_ref, first_block, second_block)


def expert_rows(pieces, first_weight, second_weight, half, kinds, staged):
    width, hidden = first_weight.shape
    count = len(pieces) * half
    scratch = [pltpu.VMEM((count, width), jnp.bfloat16), pltpu.VMEM((count, hidden), jnp.bfloat16)]
    out_shape = [jax.ShapeDtypeStruct((half, width), kind) for kind in kinds]
    specs = {}
    if staged:
        scratch += [
            pltpu.SemaphoreType.DMA((hidden // BLOCK,)),
            pltpu.SemaphoreType.DMA((width // BLOCK,)),
        ]
        out_shape += [pltpu.VMEM(w.shape, w.dtype) for w in (first_weight, second_weight)]
        near, far = pl.BlockSpec(memory_space=pltpu.VMEM), pl.BlockSpec(memory_space=pl.ANY)
        specs = {"in_specs": [near] * len(pieces) + [far] * 2, "out_specs": [near] * len(out_shape)}
    return pl.pallas_call(
        staged_expert_kernel if staged else expert_kernel,
        out_shape=out_shape,
        scratch_shapes=scratch,
        compiler_params=pltpu.CompilerParams(vmem_limit_bytes=VMEM_LIMIT),
        cost_estimate=pl.CostEstimate(
            flops=4 * count * width * hidden,
            transcendentals=0,
            bytes_accessed=4 * width * hidden + 6 * count * width,
        ),
        name="expert_rows",
        **specs,
    )(*pieces, first_weight, second_weight)


def pack_kernel(tokens_far, ranks_far, capacity_far, packed_ref, table_ref, blank_ref, *scratch):
    tokens_ref, ranks_ref, capacity_ref, sems = scratch
    experts, count = ranks_ref.shape
    width = tokens_ref.shape[1]
    capacity_copy = pltpu.make_async_copy(capacity_far, capacity_ref, sems.at[0])
    ranks_copy = pltpu.make_async_copy(ranks_far, ranks_ref, sems.at[1])
    tokens_copy = pltpu.make_async_copy(tokens_far, tokens_ref, sems.at[2])
    capacity_copy.start()
    ranks_copy.start()
    tokens_copy.start()
    blank_ref[...] = jnp.zeros(blank_ref.shape, blank_ref.dtype)
    capacity_copy.wait()
    ranks_copy.wait()
    square = (experts, experts)
    diagonal = lax.broadcasted_iota(jnp.int32, square, 0) == lax.broadcasted_iota(jnp.int32, square, 1)
    limits = jnp.broadcast_to(capacity_ref[...].astype(jnp.float32), square)
    limits = jnp.sum(jnp.where(diagonal, limits, 0.0), axis=1, keepdims=True)
    chosen = ranks_ref[...].astype(jnp.float32) < limits
    earlier = lax.broadcasted_iota(jnp.int32, (count, count), 0) < lax.broadcasted_iota(
        jnp.int32, (count, count), 1
    )
    before = jnp.dot(
        jnp.where(chosen, 1.0, 0.0).astype(jnp.bfloat16),
        jnp.where(earlier, 1.0, 0.0).astype(jnp.bfloat16),
        preferred_element_type=jnp.float32,
    )
    place = jnp.where(chosen, before, -1.0)
    row = lax.broadcasted_iota(jnp.int32, (MOST, count), 0).astype(jnp.float32)
    for e in range(experts):
        table_ref[e * MOST : (e + 1) * MOST] = jnp.where(place[e : e + 1] == row, 1.0, 0.0).astype(jnp.bfloat16)
    table = table_ref[...]
    tokens_copy.wait()
    packed = jnp.dot(table, tokens_ref[...], preferred_element_type=jnp.float32)
    packed_ref[:, :width] = packed.astype(jnp.bfloat16)
    ones = jnp.ones((count, LANES), jnp.bfloat16)
    packed_ref[:, width:] = jnp.dot(table, ones, preferred_element_type=jnp.float32).astype(jnp.bfloat16)


def pack(tokens, expert_ranks, capacity):
    count, width = tokens.shape
    rows_all = expert_ranks.shape[0] * MOST
    return pl.pallas_call(
        pack_kernel,
        out_shape=[
            jax.ShapeDtypeStruct((rows_all, width + LANES), jnp.bfloat16),
            pltpu.HBM((rows_all, count), jnp.bfloat16),
            pltpu.HBM((rows_all, width), jnp.bfloat16),
        ],
        in_specs=[pl.BlockSpec(memory_space=pl.ANY)] * 3,
        scratch_shapes=[
            pltpu.VMEM(tokens.shape, tokens.dtype),
            pltpu.VMEM(expert_ranks.shape, expert_ranks.dtype),
            pltpu.VMEM((1, *capacity.shape), capacity.dtype),
            pltpu.SemaphoreType.DMA((3,)),
        ],
        compiler_params=pltpu.CompilerParams(vmem_limit_bytes=PACK_LIMIT),
        name="pack",
    )(tokens, expert_ranks, capacity[None, :])


def place_kernel(arrived_ref, step_ref, gates_ref, top_ref, bottom_ref, here_ref):
    rows_all = arrived_ref.shape[0]
    half, width = bottom_ref.shape
    taken = arrived_ref[:, width:]
    earlier = lax.broadcasted_iota(jnp.int32, (rows_all, rows_all), 1) < lax.broadcasted_iota(
        jnp.int32, (rows_all, rows_all), 0
    )
    place = jnp.dot(
        jnp.where(earlier, 1.0, 0.0).astype(jnp.bfloat16), taken, preferred_element_type=jnp.float32
    )
    here = jnp.where(wide(taken) > 0.0, place, -1.0) - (step_ref[0] * (2 * half - 1)).astype(jnp.float32)
    here_ref[...] = here
    slots = lax.broadcasted_iota(jnp.int32, (rows_all, 2 * half), 1).astype(jnp.float32)
    table = jnp.where(here[:, :1] + 1.0 == slots, 1.0, 0.0).astype(jnp.bfloat16)
    plane = lax.dot_general(
        table, arrived_ref[:, :width], (((0,), (0,)), ((), ())), preferred_element_type=jnp.float32
    )
    count = place[rows_all - 1 :] + wide(taken[rows_all - 1 :])
    blank = jnp.zeros((1, width - gates_ref.shape[1] - LANES), jnp.float32)
    note = jnp.concatenate([gates_ref[...], count, blank], axis=1)
    row = lax.broadcasted_iota(jnp.int32, (half, width), 0)
    top_ref[...] = jnp.where(row == 0, jnp.broadcast_to(note, (half, width)), plane[:half]).astype(top_ref.dtype)
    bottom_ref[...] = plane[half:].astype(bottom_ref.dtype)


def place(arrived, step, gate_pieces, half):
    rows_all = arrived.shape[0]
    width = arrived.shape[1] - LANES
    near = pl.BlockSpec(memory_space=pltpu.VMEM)
    return pl.pallas_call(
        place_kernel,
        in_specs=[near, pl.BlockSpec(memory_space=pltpu.SMEM), near],
        out_shape=[
            jax.ShapeDtypeStruct((half, width), jnp.bfloat16),
            jax.ShapeDtypeStruct((half, width), jnp.bfloat16),
            jax.ShapeDtypeStruct((rows_all, LANES), jnp.float32),
        ],
        compiler_params=pltpu.CompilerParams(vmem_limit_bytes=VMEM_LIMIT),
        name="place",
    )(arrived, step, gate_pieces)


def finish_kernel(*refs):
    step_ref, own_ref, *refs, here_ref, kept_ref, out_ref, next_ref, most_ref, scaled_ref = refs
    parts, notes = refs[:8], [note[...].astype(jnp.float32)[:1] for note in refs[8:]]
    half = parts[0].shape[0]
    count = 2 * half
    own, step = own_ref[0], step_ref[0]
    planes = [lax.rem(own + j, len(notes)) for j in range(len(notes))]
    first = jnp.full((1, LANES), (step * (count - 1) - 1).astype(jnp.float32))
    most = jnp.zeros((1, LANES), jnp.float32)
    for plane, note in zip(planes, notes):
        rows = note[:, 3 * LANES :]
        first = first + jnp.where(plane < own, rows, 0.0)
        most = jnp.maximum(most, rows)
    next_ref[0] = step + 1
    most_ref[0] = jnp.max(most).astype(jnp.int32)
    slots = first + lax.broadcasted_iota(jnp.int32, (count, LANES), 0).astype(jnp.float32)
    lanes = lax.broadcasted_iota(jnp.int32, (1, LANES), 1)
    gates = jnp.zeros((count, LANES), jnp.float32)
    for plane, note in zip(planes, notes):
        gate = note[:, :LANES] + note[:, LANES : 2 * LANES] + note[:, 2 * LANES : 3 * LANES]
        gates = gates + jnp.where(slots == (plane * LANES + lanes).astype(jnp.float32), gate, 0.0)
    gates = jnp.sum(gates, axis=1, keepdims=True)
    quarter = half // 2
    for i, (mine, near, *fars) in enumerate((parts[:4], parts[4:])):
        for j, far in enumerate(fars):
            rows = slice(j * quarter, (j + 1) * quarter)
            sums = mine[rows] + wide(near[rows]) + wide(far[...])
            part = slice(i * half + j * quarter, i * half + (j + 1) * quarter)
            scaled_ref[part] = narrow(gates[part] * sums)
    here = here_ref[:, :1]
    places = lax.broadcasted_iota(jnp.int32, (here.shape[0], count), 1).astype(jnp.float32)
    table = jnp.where(here + 1.0 == places, 1.0, 0.0).astype(jnp.bfloat16)
    returned = jnp.dot(table, scaled_ref[...], preferred_element_type=jnp.float32)
    inside = jnp.logical_and(here >= 0.0, here < count - 1)
    out_ref[...] = narrow(jnp.where(inside, returned, wide(kept_ref[...])))


def finish(step, own_dp, parts, notes, here, kept):
    half, width = parts[0].shape
    near, scalar = pl.BlockSpec(memory_space=pltpu.VMEM), pl.BlockSpec(memory_space=pltpu.SMEM)
    corner = pl.BlockSpec((NOTE, 4 * LANES), lambda i: (0, 0))
    return pl.pallas_call(
        finish_kernel,
        grid=(1,),
        in_specs=[scalar] * 2 + [near] * len(parts) + [corner] * len(notes) + [near] * 2,
        out_specs=[near, scalar, scalar],
        out_shape=[
            jax.ShapeDtypeStruct(kept.shape, kept.dtype),
            jax.ShapeDtypeStruct((1,), jnp.int32),
            jax.ShapeDtypeStruct((1,), jnp.int32),
        ],
        scratch_shapes=[pltpu.VMEM((2 * half, width), jnp.bfloat16)],
        compiler_params=pltpu.CompilerParams(vmem_limit_bytes=VMEM_LIMIT),
        name="finish",
    )(step, own_dp, *parts, *notes, here, kept)


def ring_experts(top, bottom, first_weight, second_weight, dp_count):
    far = dp_count // 2
    half = bottom.shape[0]
    upward = [(i, (i + 1) % dp_count) for i in range(dp_count)]
    downward = [(i, (i - 1) % dp_count) for i in range(dp_count)]

    def hop(up_rows, down_rows):
        up_rows = lax.ppermute(up_rows, "dp", upward)
        down_rows = lax.ppermute(down_rows, "dp", downward)
        return up_rows, down_rows

    def mlp(*pieces, sent=(), staged=False):
        kinds = [jnp.bfloat16 if i in sent else jnp.float32 for i in range(len(pieces))]
        return expert_rows(pieces, first_weight, second_weight, half, kinds, staged)

    def after(rows, *others):
        return lax.optimization_barrier((rows, others))[0]

    notes = {0: top}
    firsts = hop(top, bottom)
    seconds = hop(bottom, top)
    *own, first_weight, second_weight = mlp(top, bottom, staged=True)
    below, above, done = {}, {}, own
    for k in range(1, far):
        firsts = after(firsts, *done)
        seconds = after(seconds, *firsts)
        notes[-k % dp_count], notes[k] = firsts[0], seconds[1]
        next_firsts = hop(*firsts)
        if k < far - 1:
            next_seconds = hop(*seconds)
            done = mlp(firsts[0], seconds[0], seconds[1], firsts[1])
            below[k], above[k] = done[:2], done[2:]
            seconds = next_seconds
        else:
            below_top, above_bottom = mlp(*firsts, sent=(0, 1))
            seconds_back = hop(above_bottom, below_top)
            seconds = after(seconds, above_bottom, below_top)
            below_bottom, above_top = mlp(*seconds)
            below[k], above[k] = (below_top, below_bottom), (above_top, above_bottom)
        firsts = next_firsts

    firsts = after(firsts, below_bottom, above_top)
    notes[far] = firsts[0]
    sends = tuple(mlp(*firsts, sent=(0, 1)))
    seconds = seconds_back
    firsts = hop(*sends)
    for k in range(far - 1, 1, -1):
        seconds = after(seconds, *sends)
        sends = narrow(wide(seconds[0]) + above[k - 1][1]), narrow(wide(seconds[1]) + below[k - 1][0])
        seconds = hop(*sends)
        firsts = after(firsts, *sends)
        if k > 2:
            sends = narrow(wide(firsts[0]) + above[k][0]), narrow(wide(firsts[1]) + below[k][1])
            firsts = hop(*sends)
    quarters = [slice(0, half // 2), slice(half // 2, half)]
    hops = []
    for part in quarters:
        sends = narrow(wide(firsts[0][part]) + above[2][0][part]), narrow(wide(firsts[1][part]) + below[2][1][part])
        hops.append(hop(*sends))
    fars = []
    for j, part in enumerate(quarters):
        firsts = after(hops[j], *sends)
        sends = narrow(wide(firsts[0]) + above[1][0][part]), narrow(wide(firsts[1]) + below[1][1][part])
        fars.append(hop(*sends))
    parts = own[0], seconds[1], fars[0][0], fars[1][0], own[1], seconds[0], fars[0][1], fars[1][1]
    return parts, [notes[j] for j in range(dp_count)]


def on_device(tokens, expert_ranks, capacity, weight_in, weight_out, gate_weights):
    dp_count = lax.axis_size("dp")
    expert_count = lax.axis_size(EXPERT)
    width = tokens.shape[1]
    slots_dp = gate_weights.shape[1]
    rows_all = expert_count * MOST
    half = (slots_dp + slots_dp // 4) // 2
    round_rows = 2 * half - 1
    own_dp = lax.axis_index("dp")

    packed, pack_table, blank = pack(tokens, expert_ranks, capacity)
    arrived = lax.all_to_all(
        packed.reshape(expert_count, MOST, width + LANES), EXPERT, split_axis=0, concat_axis=0, tiled=True
    ).reshape(rows_all, width + LANES)
    gate_high = lax.reduce_precision(gate_weights, 8, 7)
    gate_left = gate_weights - gate_high
    gate_middle = lax.reduce_precision(gate_left, 8, 7)
    gate_low = gate_left - gate_middle
    gate_pieces = jnp.concatenate([gate_high, gate_middle, gate_low], axis=1)

    def experts(state):
        step, _, sent_back = state
        top, bottom, here = place(arrived, step, gate_pieces, half)
        parts, notes = ring_experts(top, bottom, weight_in[0], weight_out[0], dp_count)
        sent_back, step, most = finish(step, own_dp.reshape(1), parts, notes, here, sent_back)
        return step, most, sent_back

    _, _, sent_back = lax.while_loop(
        lambda state: state[0][0] * round_rows < state[1][0],
        experts,
        (jnp.zeros((1,), jnp.int32), jnp.ones((1,), jnp.int32), blank),
    )
    results = lax.all_to_all(
        sent_back.reshape(expert_count, MOST, width), EXPERT, split_axis=0, concat_axis=0, tiled=True
    ).reshape(rows_all, width)
    combined = lax.dot_general(
        pack_table, results, (((0,), (0,)), ((), ())), preferred_element_type=jnp.float32
    )
    return combined.astype(jnp.bfloat16)


def solution(mesh):
    split = Mesh(
        mesh.devices.reshape(mesh.shape["dp"], 4, 4, 2), ("dp", "expert_0", "expert_1", "expert_2")
    )
    placed = (
        P(DP_EXPERT, None),
        P(None, DP_EXPERT),
        P(),
        P(EXPERT, None, "dp"),
        P(EXPERT, "dp", None),
        P(EXPERT, "dp"),
    )
    return jax.shard_map(
        on_device, mesh=split, in_specs=placed, out_specs=P(DP_EXPERT, None), check_vma=False
    )
```
